32 devices in a mesh: seq: 8 (over z, x), dp: 4 (over y, core).
Axes of the slice: x: 2, y: 2, z: 4, core: 2. Of those that a mesh axis runs over, the one named last changes fastest.
Arguments:
- conv_input: bfloat16 [4, 2048, 2816], P('dp', 'seq'), may hold values from -6 to 6
- gate_input: bfloat16 [4, 2048, 2560], P('dp', 'seq'), may hold values from -6 to 6
- step_input: float32 [4, 40, 2048], P('dp', None, 'seq'), may hold values from -7.5 to 2048
- filter_taps: float32 [4, 2816], replicated, may hold values from -3 to 3
- filter_bias: float32 [2816], replicated, may hold values from -0.5 to 0.5
- step_bias: float32 [40], replicated, may hold values from -1 to 1
- decay_log: float32 [40], replicated, may hold values from -13 to 3
- skip_gain: float32 [40], replicated, may hold values from 0.5 to 1.5
- norm_weight: float32 [2560], replicated, may hold values from 0.5 to 1.5
- output_weight: bfloat16 [2560, 1280], P('dp'), may hold values from -0.125 to 0.125
- output_grad: bfloat16 [4, 2048, 1280], P('dp', 'seq'), may hold values from -6 to 6
Outputs:
- input_grad: bfloat16 [4, 2048, 2816], P('dp', 'seq')
- gate_grad: bfloat16 [4, 2048, 2560], P('dp', 'seq')
- step_grad: float32 [4, 40, 2048], P('dp', None, 'seq')
- weight_grad: float32 [2560, 1280], P('dp')
- filter_grads: float32 [5, 2816], replicated
- norm_grad: float32 [2560], replicated
- head_grads: float32 [3, 40], replicated
The draws below stay inside these ranges and needn't reach their ends.
All inputs are finite; a program needn't handle non-finite values.
Results may differ from the reference program's by a relative error of at most 0.0029.
Values may be sent and summed in bfloat16 or wider, within the bound.
No kernel may reach another device: no remote copies, remote signals or barrier semaphores. Data moves between devices by JAX's collectives and lax.ppermute only.
A program may use at most 192 MiB of HBM per device.

```python
import jax
import jax.numpy as jnp
from jax import lax

HEADS = 40
HEAD_DIM = 64
STATE = 128
WIDTH = 1280
SPAN = 256
KERNEL = 4
TOKENS_DEV = 256
INNER = 2560
CHANNELS = 2816
SEQ_LEN = 2048
BATCH = 4


def head_rates(key):
    folded = jax.random.fold_in(key, 4099)
    slow_key, fast_key, pick_key = jax.random.split(folded, 3)
    slow_rate = jax.random.uniform(slow_key, (HEADS,), jnp.float32, 10.0, 30.0) / (0.03 * SEQ_LEN)
    fast_rate = 1.0 / (0.03 * jax.random.uniform(fast_key, (HEADS,), jnp.float32, 30.0, 50.0))
    share = 0.5
    chosen = jax.random.uniform(pick_key, (HEADS,), jnp.float32) < share
    return jnp.where(chosen, fast_rate, slow_rate)


def draw_decay_log(key, part):
    return jnp.log(head_rates(key))


def draw_step_input(key, part):
    rates = head_rates(key)
    folded = jax.random.fold_in(key, 8191)
    noise_key, block_key, place_key, loss_key = jax.random.split(folded, 4)
    noise = jax.random.uniform(noise_key, (BATCH, HEADS, SEQ_LEN), jnp.float32, -5.5, -2.5)
    levels = jax.random.uniform(block_key, (BATCH, HEADS, SEQ_LEN // TOKENS_DEV, 1), jnp.float32, -1.0, 1.0)
    spread = jnp.broadcast_to(levels, (BATCH, HEADS, SEQ_LEN // TOKENS_DEV, TOKENS_DEV)).reshape(BATCH, HEADS, SEQ_LEN)
    places = jax.random.randint(place_key, (BATCH, 2), 0, SEQ_LEN)
    marked = jnp.any(jnp.arange(SEQ_LEN)[None, None, :] == places[:, :, None], axis=1)
    losses = jax.random.uniform(loss_key, (BATCH, HEADS, 1), jnp.float32, 0.2, 0.45)
    jumps = -jnp.log(1.0 - losses) / rates[None, :, None]
    return jnp.where(marked[:, None, :], jumps, noise + spread)


def block_levels(rng, extent, cuts, least, high):
    loudness = 1.0
    for dim, parts in cuts:
        draws = jax.random.uniform(jax.random.fold_in(jax.random.fold_in(rng, 6), dim), (parts,), jnp.float32, least / len(cuts), high / len(cuts))
        loudness = loudness * jnp.repeat(jnp.exp(draws), extent[dim] // parts).reshape((-1,) + (1,) * (len(extent) - 1 - dim))
    return loudness


def scatter_about(stream_key, shape, scale, limit, cuts=(), kind=jnp.bfloat16):
    loudness = block_levels(stream_key, shape, cuts, -0.22, 0.18) if cuts else 1.0
    values = jax.random.normal(stream_key, shape, jnp.float32) * scale * loudness
    return jnp.minimum(jnp.maximum(values, -limit), limit).astype(kind)


def setup_inputs(seed: int = 0) -> dict:
    streams_of = jax.random.split(jax.random.key(seed), 12)
    return {
        "conv_input": scatter_about(streams_of[0], (BATCH, SEQ_LEN, CHANNELS), 1.0, 6.0, ((0, 4), (1, 8))),
        "gate_input": scatter_about(streams_of[1], (BATCH, SEQ_LEN, INNER), 1.0, 6.0, ((0, 4), (1, 8))),
        "step_input": draw_step_input(jax.random.fold_in(streams_of[11], 71), 0),
        "filter_taps": scatter_about(streams_of[3], (KERNEL, CHANNELS), KERNEL ** -0.5, 3.0, (), jnp.float32),
        "filter_bias": jnp.clip(jax.random.uniform(streams_of[4], (CHANNELS,), jnp.float32, -0.5, 0.5), -0.5, 0.5),
        "step_bias": jnp.clip(jax.random.uniform(streams_of[5], (HEADS,), jnp.float32, -1.0, 1.0), -1.0, 1.0),
        "decay_log": draw_decay_log(jax.random.fold_in(streams_of[11], 71), 0),
        "skip_gain": jnp.clip(jax.random.uniform(streams_of[7], (HEADS,), jnp.float32, 0.5, 1.5), 0.5, 1.5),
        "norm_weight": jnp.clip(1.0 + 0.1 * jax.random.normal(streams_of[8], (INNER,), jnp.float32), 0.5, 1.5),
        "output_weight": scatter_about(streams_of[9], (INNER, WIDTH), INNER ** -0.5, 0.125, ((0, 4),)),
        "output_grad": scatter_about(streams_of[10], (BATCH, SEQ_LEN, WIDTH), 1.0, 6.0, ((0, 4), (1, 8))),
    }


HIGHEST = lax.Precision.HIGHEST
MASKED = -1e+30
EPSILON = 1e-05

def block_step(skip_gain, carried, slices):
    activated, block_steps, block_rates = slices
    length = activated.shape[0]
    values = activated[:, :INNER].reshape(length, HEADS, HEAD_DIM)
    key_side = activated[:, INNER:INNER + STATE]
    query_side = activated[:, INNER + STATE:]
    cumsums = jnp.cumsum(block_rates, axis=1)
    scaled = values * block_steps.T[:, :, None]
    to_end = jnp.exp(cumsums[:, -1:] - cumsums)
    block_state = jnp.einsum('hs,shp,sn->hpn', to_end, scaled, key_side, precision=HIGHEST)
    scores = jnp.einsum('tn,sn->ts', query_side, key_side, precision=HIGHEST)
    differences = cumsums[:, :, None] - cumsums[:, None, :]
    causal = jnp.tril(jnp.ones((length, length), dtype=bool))
    weights = scores[None] * jnp.exp(jnp.where(causal[None], differences, MASKED))
    inside = jnp.einsum('hts,shp->thp', weights, scaled, precision=HIGHEST)
    from_state = jnp.einsum('tn,hpn->thp', query_side, carried, precision=HIGHEST) * jnp.exp(cumsums).T[:, :, None]
    result = inside + from_state + skip_gain[:, None] * values
    updated = jnp.exp(cumsums[:, -1])[:, None, None] * carried + block_state
    return (updated, result.reshape(length, INNER))

def layer_forward(raw_rows, gate_rows, step_rows, filter_taps, filter_bias, step_bias, decay_log, skip_gain, norm_weight):
    length = raw_rows.shape[0]
    padded = jnp.concatenate([jnp.zeros((KERNEL - 1, CHANNELS), jnp.float32), raw_rows], axis=0)
    filtered = filter_bias + filter_taps[0] * padded[0:length]
    for offset in range(1, KERNEL):
        filtered = filtered + filter_taps[offset] * padded[offset:offset + length]
    activated = jax.nn.silu(filtered)
    step_sizes = jax.nn.softplus(step_rows + step_bias[:, None])
    decay_rates = step_sizes * (-jnp.exp(decay_log))[:, None]
    blocks = length // SPAN
    pieces = (activated.reshape(blocks, SPAN, CHANNELS), step_sizes.reshape(HEADS, blocks, SPAN).transpose(1, 0, 2), decay_rates.reshape(HEADS, blocks, SPAN).transpose(1, 0, 2))
    stepper = jax.checkpoint(lambda carried, slices: block_step(skip_gain, carried, slices))
    _, outputs = lax.scan(stepper, jnp.zeros((HEADS, HEAD_DIM, STATE), jnp.float32), pieces)
    scanned = outputs.reshape(length, INNER)
    gated = scanned * jax.nn.silu(gate_rows)
    inverse_rms = lax.rsqrt(lax.optimization_barrier(jnp.mean(gated * gated, axis=1, keepdims=True)) + EPSILON)
    return gated * inverse_rms * norm_weight

def reference(conv_input, gate_input, step_input, filter_taps, filter_bias, step_bias, decay_log, skip_gain, norm_weight, output_weight, output_grad):

    def one_sequence(slices):
        raw_rows, gate_rows, step_rows, cotangent = slices
        normed, pullback = jax.vjp(layer_forward, raw_rows.astype(jnp.float32), gate_rows.astype(jnp.float32), step_rows, filter_taps, filter_bias, step_bias, decay_log, skip_gain, norm_weight)
        normed_low = normed.astype(jnp.bfloat16)
        normed_grad = jnp.dot(cotangent, output_weight.T, preferred_element_type=jnp.float32)
        weight_term = jnp.dot(normed_low.T, cotangent, preferred_element_type=jnp.float32)
        return tuple(pullback(normed_grad)) + (weight_term,)
    results = lax.map(one_sequence, (conv_input, gate_input, step_input, output_grad))
    input_grad = results[0].astype(jnp.bfloat16)
    gate_grad = results[1].astype(jnp.bfloat16)
    step_grad = results[2]
    filter_grads = jnp.concatenate([lax.optimization_barrier(jnp.sum(results[3], axis=0)), lax.optimization_barrier(jnp.sum(results[4], axis=0))[None]], axis=0)
    head_grads = jnp.stack([lax.optimization_barrier(jnp.sum(results[5], axis=0)), lax.optimization_barrier(jnp.sum(results[6], axis=0)), lax.optimization_barrier(jnp.sum(results[7], axis=0))])
    norm_grad = lax.optimization_barrier(jnp.sum(results[8], axis=0))
    weight_grad = lax.optimization_barrier(jnp.sum(results[9], axis=0))
    return (input_grad, gate_grad, step_grad, weight_grad, filter_grads, norm_grad, head_grads)
```

```python
import functools

import jax
import jax.numpy as jnp
from jax import lax
from jax.experimental import pallas as pl
from jax.experimental.pallas import tpu as pltpu
from jax.sharding import PartitionSpec as P

F32 = jnp.float32
BF16 = jnp.bfloat16
HIGHEST = lax.Precision.HIGHEST
MASKED = -1e30
EPSILON = 1e-05
PAIR = 128
CODE = 120.0
TINY = 1e-30
VMEM = 60 * 1024 * 1024


NN = (((1,), (0,)), ((), ()))
NT = (((1,), (1,)), ((), ()))


def params(limit=VMEM):
    return pltpu.CompilerParams(dimension_semantics=("arbitrary",), vmem_limit_bytes=limit)


def cost(flops, nbytes):
    return pl.CostEstimate(flops=int(flops), bytes_accessed=int(nbytes), transcendentals=0)


def full(shape):
    zeros = (0,) * len(shape)
    return pl.BlockSpec(shape, lambda *_: zeros)


SMEM = pl.BlockSpec(memory_space=pltpu.SMEM)


def dot(a, b, dims):
    return lax.dot_general(a, b, dims, preferred_element_type=F32)


def split(x):
    high = x.astype(BF16)
    return high, (x - high.astype(F32)).astype(BF16)


def dot3(a, b, dims):
    (ah, al), (bh, bl) = a, b
    return dot(ah, bh, dims) + dot(ah, bl, dims) + dot(al, bh, dims)


def both(first, second, rows):
    width = first.shape[-1]
    return jnp.concatenate(
        [jnp.broadcast_to(first, (rows, width)), jnp.broadcast_to(second, (rows, width))], axis=0
    )


def choose(index, parts):
    out = parts[0]
    for k in range(1, len(parts)):
        out = jnp.where(index == k, parts[k], out)
    return out


def triangle(size, upper):
    row = lax.broadcasted_iota(jnp.int32, (size, size), 0)
    col = lax.broadcasted_iota(jnp.int32, (size, size), 1)
    return row <= col if upper else row >= col


def steps_kernel(step_ref, bias_ref, log_ref, steps_ref, cums_ref, decay_ref):
    raw = step_ref[...] + bias_ref[...]
    steps = jnp.maximum(raw, 0.0) + jnp.log1p(jnp.exp(-jnp.abs(raw)))
    rates = -jnp.exp(log_ref[...]) * steps
    size = raw.shape[1]
    ones = jnp.where(triangle(size, True), 1.0, 0.0).astype(F32)
    cums = lax.dot_general(rates, ones, NN, precision=HIGHEST, preferred_element_type=F32)
    steps_ref[...] = steps
    cums_ref[...] = cums
    heads = raw.shape[0]
    last = jnp.exp(cums[:, size - 1 :])
    row = lax.broadcasted_iota(jnp.int32, (heads, decay_ref.shape[1]), 0)
    col = lax.broadcasted_iota(jnp.int32, (heads, decay_ref.shape[1]), 1)
    decay_ref[...] = jnp.sum(jnp.where(row == col, last, 0.0), axis=0, keepdims=True)


def filter_kernel(
    halo_ref, raw_ref, taps_ref, bias_ref, steps_ref, cums_ref,
    slope_ref, features_ref, sides_ref, state_ref, key_high, key_low,
):
    i = pl.program_id(0)
    raw = raw_ref[...].astype(F32)
    size = raw.shape[0]
    extended = jnp.concatenate([halo_ref[...].astype(F32), raw], axis=0)
    taps = taps_ref[...]
    width = taps.shape[0]
    start = halo_ref.shape[0] - width + 1
    filtered = bias_ref[...] + taps[0:1] * extended[start : start + size]
    for k in range(1, width):
        filtered = filtered + taps[k : k + 1] * extended[start + k : start + k + size]
    gate = jax.nn.sigmoid(filtered)
    active = filtered * gate
    slope_ref[...] = gate + active * (1.0 - gate)
    features = active.T
    features_ref[...] = features

    @pl.when(i < 2)
    def _():
        sides_ref[...] = active

    @pl.when(i == 0)
    def _():
        high, low = split(active)
        key_high[...] = high
        key_low[...] = low

    @pl.when(i >= 2)
    def _():
        head = jnp.maximum(i - 2, 0) * 2
        rows = []
        for j in range(2):
            cums = cums_ref[pl.ds(head + j, 1), :]
            rows.append(steps_ref[pl.ds(head + j, 1), :] * jnp.exp(cums[:, size - 1 :] - cums))
        scaled = features * both(rows[0], rows[1], PAIR // 2)
        keys = (key_high[...], key_low[...])
        state_ref[...] = dot3(split(scaled), keys, NN).astype(BF16)


def carry_kernel(group, reverse, width, me_ref, decays_ref, *refs):
    parts, out_ref = refs[:-1], refs[-1]
    scan_chunk(group, reverse, width, me_ref, decays_ref, parts, None, None, out_ref)


def spread_kernel(group, reverse, width, me_ref, decays_ref, carry_ref, *refs):
    parts, outs, scratch = refs[:group], refs[group : 2 * group], refs[2 * group]
    scan_chunk(group, reverse, width, me_ref, decays_ref, parts, carry_ref, scratch, None)
    here = me_ref[0] % group
    for k in range(group):
        outs[k][...] = scratch[here ^ k].astype(BF16)


def scan_chunk(group, reverse, width, me_ref, decays_ref, parts, carry_ref, scratch, total_ref):
    here = me_ref[0] % group
    heads = parts[0].shape[0] // width
    order = range(group - 1, -1, -1) if reverse else range(group)
    for h in range(heads):
        rows = pl.ds(h * width, width)
        if carry_ref is None:
            running = jnp.zeros((width, parts[0].shape[1]), F32)
        else:
            running = carry_ref[rows, :].astype(F32)
        for n, p in enumerate(order):
            if scratch is not None:
                scratch[p, rows, :] = running
                if n == group - 1:
                    break
            slot = here ^ p
            term = choose(slot, [part[rows, :] for part in parts]).astype(F32)
            running = term + decays_ref[slot, here * heads + h] * running
        if total_ref is not None:
            total_ref[rows, :] = running.astype(BF16)


def exchange(state, decays, me, seq, group, head_dim, reverse):
    groups = seq // group
    rows = state.shape[0] // group
    here = me[0] % group
    chunks = [
        lax.dynamic_slice_in_dim(state, (here ^ k) * rows, rows, axis=0) for k in range(group)
    ]
    got = [chunks[0]]
    for k in range(1, group):
        got.append(lax.ppermute(chunks[k], "seq", [(s, s ^ k) for s in range(seq)]))
    shape = got[0].shape
    piece = jax.ShapeDtypeStruct(shape, BF16)
    carry = None
    ways = [(s, s - group) for s in range(group, seq)] if reverse else [
        (s, s + group) for s in range(seq - group)
    ]
    if groups > 1:
        total = pl.pallas_call(
            functools.partial(carry_kernel, group, reverse, head_dim),
            out_shape=piece,
            in_specs=[SMEM, SMEM] + [full(shape)] * group,
            out_specs=full(shape),
            grid=(1,),
            compiler_params=params(),
            cost_estimate=cost(2e6, 1e6),
            name="scan_total",
        )(me, decays, *got)
        carry = lax.ppermute(total, "seq", ways)
        if groups > 2:
            row_heads = here * (rows // head_dim) + jnp.arange(rows) // head_dim
            product = jnp.take(jnp.prod(decays[:group], axis=0), row_heads)[:, None]
            for _ in range(groups - 2):
                step = total.astype(F32) + product * carry.astype(F32)
                carry = lax.ppermute(step.astype(BF16), "seq", ways)
    else:
        carry = jnp.zeros(shape, BF16)
    outs = pl.pallas_call(
        functools.partial(spread_kernel, group, reverse, head_dim),
        out_shape=[piece] * group,
        in_specs=[SMEM, SMEM] + [full(shape)] * (group + 1),
        out_specs=[full(shape)] * group,
        grid=(1,),
        scratch_shapes=[pltpu.VMEM((group,) + shape, F32)],
        compiler_params=params(),
        cost_estimate=cost(4e6, 2e6),
        name="scan_spread",
    )(me, decays, carry, *got)
    back = [outs[0]]
    for k in range(1, group):
        back.append(lax.ppermute(outs[k], "seq", [(s, s ^ k) for s in range(seq)]))
    return back


def weights_of(score, row, column, causal):
    return score * jnp.exp(jnp.where(causal, row - column, MASKED))


def inside_kernel(
    skip_ref, features_ref, sides_ref, steps_ref, cums_ref, columns_ref, out_ref, score_ref
):
    i = pl.program_id(0)

    @pl.when(i == 0)
    def _():
        sides = sides_ref[...]
        state = sides.shape[1] // 2
        score_ref[...] = dot3(split(sides[:, :state]), split(sides[:, state:]), NT)

    size = score_ref.shape[0]
    causal = triangle(size, True)
    half = PAIR // 2
    for j in range(2):
        head = 2 * i + j
        values = features_ref[j * half : (j + 1) * half, :]
        scaled = values * steps_ref[pl.ds(head, 1), :]
        row = cums_ref[pl.ds(head, 1), :]
        weights = weights_of(score_ref[...], row, columns_ref[0][:, j : j + 1], causal)
        wh, wl = split(weights)
        xh, xl = split(scaled)
        first = dot(jnp.concatenate([xh, xl], axis=0), wh, NN)
        inside = first[:half] + first[half:] + dot(xh, wl, NN)
        out_ref[j * half : (j + 1) * half, :] = inside + skip_ref[head] * values


def norm_kernel(
    pieces, me_ref, *refs
):
    seq_group, dp_group = pieces
    states, refs = refs[:seq_group], refs[seq_group:]
    grads, refs = refs[:dp_group], refs[dp_group:]
    (
        local_ref, gate_ref, cums_ref, sides_ref, query_ref, weight_ref,
        scanned_ref, low_ref, cotangent_ref, entry_ref, gate_grad_ref, norm_ref,
        entering_ref, gated_s, open_s, grad_s, square_s, cross_s,
    ) = refs
    phase, b = pl.program_id(0), pl.program_id(1)
    half = PAIR // 2
    here = pl.ds(b * PAIR, PAIR)
    size = local_ref.shape[1]
    blocks = pl.num_programs(1)
    exps = both(
        jnp.exp(cums_ref[pl.ds(2 * b, 1), :]), jnp.exp(cums_ref[pl.ds(2 * b + 1, 1), :]), half
    )

    @pl.when(phase == 0)
    def _():
        rows = states[0].shape[0]
        owner = (b * PAIR) // rows
        at = pl.ds(pl.multiple_of(b * PAIR - owner * rows, PAIR), PAIR)
        entering = choose((me_ref[0] % seq_group) ^ owner, [s[at, :] for s in states])
        entering_ref[...] = entering
        query = query_ref[...]
        qh, ql = split(query)
        carried = dot(entering, qh, NN) + dot(entering, ql, NN)
        scanned = local_ref[...] + carried * exps
        scanned_ref[here, :] = scanned
        z = gate_ref[...].astype(F32).T
        opened = jax.nn.sigmoid(z)
        gated = scanned * (z * opened)
        width = grads[0].shape[0] - 16
        source = (b * PAIR) // width
        start = pl.multiple_of(b * PAIR - source * width, PAIR)
        slot = me_ref[1] ^ source
        coded = choose(slot, [g[pl.ds(start, PAIR), :] for g in grads])
        scale = choose(slot, [g[width : width + 1, :] for g in grads])
        grad = jnp.log2(coded.astype(F32)) * (scale.astype(F32) * (1.0 / CODE))
        gated_s[here, :] = gated
        open_s[here, :] = opened
        grad_s[here, :] = grad
        square = jnp.sum(gated * gated, axis=0, keepdims=True)
        cross = jnp.sum(gated * (grad * weight_ref[...]), axis=0, keepdims=True)

        @pl.when(b == 0)
        def _():
            square_s[...] = square
            cross_s[...] = cross

        @pl.when(b > 0)
        def _():
            square_s[...] += square
            cross_s[...] += cross

    @pl.when(phase == 1)
    def _():
        inner = 1.0 / (blocks * PAIR)
        inverse = lax.rsqrt(square_s[...] * inner + EPSILON)
        shift = inverse * inverse * inverse * (cross_s[...] * inner)
        gated, opened, grad = gated_s[here, :], open_s[here, :], grad_s[here, :]
        weight = weight_ref[...]
        unit = gated * inverse
        low_ref[...] = (unit * weight).astype(BF16)
        product = split(unit * grad)
        ones = jnp.ones((8, size), BF16)
        norm_ref[...] = dot(ones, product[0], NT) + dot(ones, product[1], NT)
        gated_grad = inverse * (grad * weight) - gated * shift
        z = gate_ref[...].astype(F32).T
        through = z * opened
        cotangent = gated_grad * through
        cotangent_ref[...] = cotangent
        gate_grad = gated_grad * scanned_ref[here, :] * (opened + through * (1.0 - opened))
        gate_grad_ref[...] = gate_grad.T.astype(BF16)
        entry_ref[...] = dot3(split(cotangent * exps), split(sides_ref[...]), NN).astype(BF16)


def inner_kernel(
    skip_ref, features_ref, sides_ref, key_ref, query_ref, steps_ref, cums_ref, columns_ref,
    cotangent_ref, scanned_ref, entering_ref,
    grad_ref, side_grad_ref, row_ref, direct_ref,
    score_ref, total_ref, carried_ref,
):
    i = pl.program_id(0)
    sides = sides_ref[...]
    state = sides.shape[1] // 2

    @pl.when(i == 0)
    def _():
        score_ref[...] = dot3(split(sides[:, :state]), split(sides[:, state:]), NT)
        total_ref[...] = jnp.zeros_like(total_ref)
        carried_ref[...] = jnp.zeros_like(carried_ref)

    size = score_ref.shape[0]
    causal = triangle(size, True)
    half = PAIR // 2
    for j in range(2):
        head = 2 * i + j
        part = slice(j * half, (j + 1) * half)
        values = features_ref[part, :]
        cotangent = cotangent_ref[part, :]
        scaled = values * steps_ref[pl.ds(head, 1), :]
        row = cums_ref[pl.ds(head, 1), :]
        decay = jnp.exp(jnp.where(causal, row - columns_ref[0][:, j : j + 1], MASKED))
        wh, wl = split(score_ref[...] * decay)
        gh, gl = split(cotangent)
        xh, xl = split(scaled.T)
        first = dot(jnp.concatenate([gh, gl], axis=0), wh, NT)
        grad_ref[part, :] = first[:half] + first[half:] + dot(gh, wl, NT)
        left = jnp.concatenate([xh, xh, xl], axis=1)
        right = jnp.concatenate([gh, gl, gh], axis=0)
        total_ref[...] += dot(left, right, NN) * decay
        direct = cotangent * values
        skip = skip_ref[head]
        row_ref[pl.ds(head, 1), :] = jnp.sum(
            cotangent * scanned_ref[part, :] - skip * direct, axis=0, keepdims=True
        )
        direct_ref[pl.ds(head, 1), :] = jnp.sum(direct, axis=0, keepdims=True)
    exps = both(
        jnp.exp(cums_ref[pl.ds(2 * i, 1), :]), jnp.exp(cums_ref[pl.ds(2 * i + 1, 1), :]), half
    )
    ch, cl = split(cotangent_ref[...] * exps)
    entering = entering_ref[...].astype(F32).T.astype(BF16)
    carried_ref[...] += dot(entering, ch, NN) + dot(entering, cl, NN)

    @pl.when(i == pl.num_programs(0) - 1)
    def _():
        total = split(total_ref[...])
        side_grad_ref[:state, :] = dot3(split(query_ref[...]), total, NT)
        side_grad_ref[state:, :] = dot3(split(key_ref[...]), total, NN) + carried_ref[...]


def outer_kernel(
    pieces, me_ref, skip_ref, *refs
):
    states, refs = refs[:pieces], refs[pieces:]
    (
        features_ref, key_ref, steps_ref, cums_ref, cotangent_ref, grad_ref, side_grad_ref,
        entering_ref, row_ref, direct_ref, step_in_ref, bias_ref, log_ref, norm_ref,
        slope_ref, raw_ref, halo_ref, taps_ref,
        out_ref, tail_ref, back_ref, sums_ref, step_ref,
        key_grad_s, value_s, end_s, decay_s,
    ) = refs
    i = pl.program_id(0)
    blocks = pl.num_programs(0) - 2
    half = PAIR // 2
    size = raw_ref.shape[0]
    heads = steps_ref.shape[0]
    sides = key_ref.shape[0]

    @pl.when(i == 0)
    def _():
        key_grad_s[...] = jnp.zeros_like(key_grad_s)

    def filtered(grad):
        df = grad.T * slope_ref[...]
        taps = taps_ref[...]
        width = taps.shape[0]
        longer = jnp.concatenate([df, jnp.zeros((8, PAIR), F32)], axis=0)
        ahead = jnp.concatenate([jnp.zeros((8, PAIR), F32), df[0:8]], axis=0)
        extended = jnp.concatenate([halo_ref[...].astype(F32), raw_ref[...].astype(F32)], axis=0)
        start = halo_ref.shape[0] - width + 1
        last = width - 1
        own = taps[0:1] * longer[last : last + size]
        back = taps[0:1] * ahead[last : last + 8]
        sums = [jnp.sum(df * extended[start : start + size], axis=0, keepdims=True)]
        for k in range(1, width):
            own = own + taps[k : k + 1] * longer[last - k : last - k + size]
            back = back + taps[k : k + 1] * ahead[last - k : last - k + 8]
            sums.append(
                jnp.sum(df * extended[start + k : start + k + size], axis=0, keepdims=True)
            )
        sums.append(jnp.sum(df, axis=0, keepdims=True))
        out_ref[...] = own.astype(BF16)
        tail_ref[...] = own[size - 8 :]
        back_ref[...] = back
        sums_ref[...] = jnp.concatenate(
            sums + [jnp.zeros((8 - len(sums), PAIR), F32)], axis=0
        )

    @pl.when(i < blocks)
    def _():
        b = jnp.minimum(i, blocks - 1)
        rows = states[0].shape[0]
        owner = (b * PAIR) // rows
        at = pl.ds(pl.multiple_of(b * PAIR - owner * rows, PAIR), PAIR)
        ending = choose((me_ref[0] % pieces) ^ owner, [s[at, :] for s in states])
        kh, kl = split(key_ref[...])
        from_end = dot(ending, kh, NN) + dot(ending, kl, NN)
        tops, steps = [], []
        for j in range(2):
            cums = cums_ref[pl.ds(2 * b + j, 1), :]
            tops.append(jnp.exp(cums[:, size - 1 :] - cums))
            steps.append(steps_ref[pl.ds(2 * b + j, 1), :])
        top = both(tops[0], tops[1], half)
        step = both(steps[0], steps[1], half)
        values = features_ref[...]
        from_end = from_end * top
        grad = grad_ref[...] + from_end
        scaled = values * step
        sh, sl = split(scaled * top)
        ends = ending.astype(F32).T.astype(BF16)
        key_grad_s[...] += dot(ends, sh, NN) + dot(ends, sl, NN)
        by_value = values * grad
        by_end = scaled * from_end
        product = ending.astype(F32) * entering_ref[...].astype(F32)
        skips = []
        for j in range(2):
            part = slice(j * half, (j + 1) * half)
            at = pl.ds(2 * b + j, 1)
            value_s[at, :] = jnp.sum(by_value[part], axis=0, keepdims=True)
            end_s[at, :] = jnp.sum(by_end[part], axis=0, keepdims=True)
            decay_s[at, :] = jnp.sum(product[part], axis=0, keepdims=True)
            skips.append(skip_ref[2 * b + j] * cotangent_ref[part, :])
        filtered(jnp.concatenate(skips, axis=0) + grad * step)
        sums_ref[5:6, :] = norm_ref[0:1, :]

    @pl.when(i == blocks)
    def _():
        filtered(side_grad_ref[:sides, :] + key_grad_s[...])

    @pl.when(i == blocks + 1)
    def _():
        filtered(side_grad_ref[sides:, :])
        steps, cums = steps_ref[...], cums_ref[...]
        values = value_s[...]
        base = row_ref[...] - steps * values
        ones = jnp.where(triangle(size, False), 1.0, 0.0).astype(F32)
        rate_grad = lax.dot_general(base, ones, NN, precision=HIGHEST, preferred_element_type=F32)
        ended = jnp.sum(end_s[...], axis=1, keepdims=True)
        kept = jnp.exp(cums[:, size - 1 :]) * jnp.sum(decay_s[...], axis=1, keepdims=True)
        rate_grad = rate_grad + (ended + kept)
        rate = -jnp.exp(log_ref[...])
        step_grad = (values + rate_grad * rate) * jax.nn.sigmoid(step_in_ref[...] + bias_ref[...])
        step_ref[...] = step_grad
        row = lax.broadcasted_iota(jnp.int32, (heads, PAIR), 0)
        col = lax.broadcasted_iota(jnp.int32, (heads, PAIR), 1)
        for k, source in enumerate((step_grad, rate_grad * steps * rate, direct_ref[...])):
            column = jnp.sum(source, axis=1, keepdims=True)
            sums_ref[5 + k : 6 + k, :] = jnp.sum(
                jnp.where(row == col, column, 0.0), axis=0, keepdims=True
            )


def encode(values):
    scale = jnp.max(jnp.abs(values), axis=0, keepdims=True) * 1.01 + TINY
    scale = scale.astype(BF16)
    coded = jnp.exp2(values * (CODE / scale.astype(F32))).astype(BF16)
    return coded, jnp.broadcast_to(scale, (16, values.shape[1]))


def project_kernel(count, weight_ref, *refs):
    cotangents, outs = refs[:count], refs[count:]
    rows = weight_ref.shape[0]
    for k in range(count):
        coded, scale = encode(dot(weight_ref[...], cotangents[k][...], NT))
        outs[k][:rows, :] = coded
        outs[k][rows:, :] = scale


def outer_product_kernel(count, *refs):
    lows, cotangents, out_ref = refs[:count], refs[count : 2 * count], refs[2 * count]
    total = dot(lows[0][...], cotangents[0][...], NN)
    for k in range(1, count):
        total = total + dot(lows[k][...], cotangents[k][...], NN)
    out_ref[...] = total


def encode_kernel(values_ref, out_ref):
    coded, scale = encode(values_ref[...])
    rows = values_ref.shape[0]
    out_ref[:rows, :] = coded
    out_ref[rows:, :] = scale


def decode_kernel(me_ref, coded_ref, out_ref):
    rows = out_ref.shape[1]
    coded = coded_ref[0, :rows, :].astype(F32)
    scale = coded_ref[0, rows : rows + 1, :].astype(F32)
    out_ref[0] = jnp.log2(coded) * (scale * (1.0 / CODE))


def body(
    conv_input, gate_input, step_input, filter_taps, filter_bias, step_bias, decay_log,
    skip_gain, norm_weight, output_weight, output_grad,
):
    seq, dp = lax.axis_size("seq"), lax.axis_size("dp")
    me = jnp.stack([lax.axis_index("seq"), lax.axis_index("dp")]).astype(jnp.int32)
    group = min(4, seq)
    raw, gate, step_rows, cotangent = conv_input[0], gate_input[0], step_input[0], output_grad[0]
    tokens, channels = raw.shape
    inner = gate.shape[1]
    heads = step_rows.shape[0]
    head_dim = inner // heads
    state = (channels - inner) // 2
    width = cotangent.shape[1]
    blocks = inner // PAIR
    both_axes = ("seq", "dp")

    def swap(value, seq_bits, dp_bits):
        pairs = [
            (s * dp + d, (s ^ seq_bits) * dp + (d ^ dp_bits)) for s in range(seq) for d in range(dp)
        ]
        return lax.ppermute(value, both_axes, pairs)

    halo = lax.ppermute(raw[-8:], "seq", [(s, s + 1) for s in range(seq - 1)])

    known = {(0, 0): cotangent}
    bit = dp // 2
    while bit:
        for key in list(known):
            known[(0, key[1] | bit)] = swap(known[key], 0, bit)
        bit //= 2
    side_bits = 1 if seq > 1 else 0

    column = lambda v: v.reshape(-1, 1)
    steps, cums, decay = pl.pallas_call(
        steps_kernel,
        out_shape=[
            jax.ShapeDtypeStruct((heads, tokens), F32),
            jax.ShapeDtypeStruct((heads, tokens), F32),
            jax.ShapeDtypeStruct((1, PAIR), F32),
        ],
        name="steps",
        cost_estimate=cost(2e7, 2e5),
    )(step_rows, column(step_bias), column(decay_log))
    decays = decay
    bit = 1
    while bit < group:
        decays = jnp.concatenate([decays, swap(decays, bit, 0)], axis=0)
        bit *= 2

    order = lambda i: jnp.where(i < 2, blocks + i, i - 2)
    heads_spec = full((heads, tokens))
    slope, features, sides, block_state = pl.pallas_call(
        filter_kernel,
        grid=(blocks + 2,),
        in_specs=[
            pl.BlockSpec((8, PAIR), lambda i: (0, order(i))),
            pl.BlockSpec((tokens, PAIR), lambda i: (0, order(i))),
            pl.BlockSpec((filter_taps.shape[0], PAIR), lambda i: (0, order(i))),
            pl.BlockSpec((1, PAIR), lambda i: (0, order(i))),
            heads_spec,
            heads_spec,
        ],
        out_specs=[
            pl.BlockSpec((tokens, PAIR), lambda i: (0, order(i))),
            pl.BlockSpec((PAIR, tokens), lambda i: (order(i), 0)),
            pl.BlockSpec((tokens, state), lambda i: (0, jnp.minimum(i, 1))),
            pl.BlockSpec((PAIR, state), lambda i: (jnp.maximum(i - 2, 0), 0)),
        ],
        out_shape=[
            jax.ShapeDtypeStruct((tokens, channels), F32),
            jax.ShapeDtypeStruct((channels, tokens), F32),
            jax.ShapeDtypeStruct((tokens, 2 * state), F32),
            jax.ShapeDtypeStruct((inner, state), BF16),
        ],
        scratch_shapes=[pltpu.VMEM((tokens, state), BF16)] * 2,
        compiler_params=params(),
        cost_estimate=cost(1e9, 1e7),
        name="filter",
    )(halo, raw, filter_taps, filter_bias.reshape(1, -1), steps, cums)

    entering = exchange(block_state, decays, me, seq, group, head_dim, False)

    columns = cums.reshape(blocks, 2, tokens).transpose(0, 2, 1)
    pair_spec = pl.BlockSpec((PAIR, tokens), lambda i: (i, 0))
    column_spec = pl.BlockSpec((1, tokens, 2), lambda i: (i, 0, 0))
    sides_spec = full((tokens, 2 * state))
    local = pl.pallas_call(
        inside_kernel,
        grid=(blocks,),
        in_specs=[SMEM, pair_spec, sides_spec, heads_spec, heads_spec, column_spec],
        out_specs=pair_spec,
        out_shape=jax.ShapeDtypeStruct((inner, tokens), F32),
        scratch_shapes=[pltpu.VMEM((tokens, tokens), F32)],
        compiler_params=params(),
        cost_estimate=cost(8e9, 6e6),
        name="inside",
    )(skip_gain, features, sides, steps, cums, columns)

    own_rows = output_weight.shape[0]
    piece = jax.ShapeDtypeStruct((own_rows + 16, tokens), BF16)
    served = pl.pallas_call(
        functools.partial(project_kernel, dp),
        out_shape=[piece] * dp,
        compiler_params=pltpu.CompilerParams(vmem_limit_bytes=VMEM),
        cost_estimate=cost(4e9, 8e6),
        name="project",
    )(output_weight, *[known[(0, k)] for k in range(dp)])
    grads = [served[0]] + [swap(served[k], 0, k) for k in range(1, dp)]
    if side_bits:
        for k in range(dp):
            if k % 2 == 0:
                known[(1, k)] = swap(known[(0, k)], 1, 0)
        for k in range(dp):
            if k % 2 == 1:
                known[(1, k)] = swap(known[(1, k - 1)], 0, 1)

    rows = entering[0].shape[0]
    norm_out = lambda p, b: jnp.where(p == 1, b, 0)
    norm_in = lambda p, b: jnp.where(p == 0, b, blocks - 1)
    scanned, low, scan_grad, entry, gate_grad, norm_grad, entered = pl.pallas_call(
        functools.partial(norm_kernel, (group, dp)),
        grid=(2, blocks),
        in_specs=[SMEM]
        + [full((rows, state))] * group
        + [full(piece.shape)] * dp
        + [
            pl.BlockSpec((PAIR, tokens), lambda p, b: (norm_in(p, b), 0)),
            pl.BlockSpec((tokens, PAIR), lambda p, b: (0, b)),
            heads_spec,
            pl.BlockSpec((tokens, state), lambda p, b: (0, 1)),
            pl.BlockSpec((state, tokens), lambda p, b: (blocks + 1, 0)),
            pl.BlockSpec((PAIR, 1), lambda p, b: (b, 0)),
        ],
        out_specs=[
            full((inner, tokens)),
            pl.BlockSpec((PAIR, tokens), lambda p, b: (norm_out(p, b), 0)),
            pl.BlockSpec((PAIR, tokens), lambda p, b: (norm_out(p, b), 0)),
            pl.BlockSpec((PAIR, state), lambda p, b: (norm_out(p, b), 0)),
            pl.BlockSpec((tokens, PAIR), lambda p, b: (0, norm_out(p, b))),
            pl.BlockSpec((8, PAIR), lambda p, b: (0, norm_out(p, b))),
            pl.BlockSpec((PAIR, state), lambda p, b: (norm_in(p, b), 0)),
        ],
        out_shape=[
            jax.ShapeDtypeStruct((inner, tokens), F32),
            jax.ShapeDtypeStruct((inner, tokens), BF16),
            jax.ShapeDtypeStruct((inner, tokens), F32),
            jax.ShapeDtypeStruct((inner, state), BF16),
            jax.ShapeDtypeStruct((tokens, inner), BF16),
            jax.ShapeDtypeStruct((8, inner), F32),
            jax.ShapeDtypeStruct((inner, state), BF16),
        ],
        scratch_shapes=[pltpu.VMEM((inner, tokens), F32)] * 3 + [pltpu.VMEM((1, tokens), F32)] * 2,
        compiler_params=pltpu.CompilerParams(
            dimension_semantics=("arbitrary", "arbitrary"), vmem_limit_bytes=VMEM
        ),
        cost_estimate=cost(3e9, 2e7),
        name="norm",
    )(me, *entering, *grads, local, gate, cums, sides, features, column(norm_weight))

    ending = exchange(entry, decays, me, seq, group, head_dim, True)

    sides_count = 2 if side_bits else 1
    part_rows = own_rows // sides_count
    lows, pairs = [], []
    for ks in range(sides_count):
        for kd in range(dp):
            at = ((me[1] ^ kd) * sides_count + ((me[0] & side_bits) ^ ks)) * part_rows
            chunk = lax.dynamic_slice_in_dim(low, at, part_rows, axis=0)
            lows.append(chunk if ks == kd == 0 else swap(chunk, ks, kd))
            pairs.append(known[(ks, kd)])
    partial = pl.pallas_call(
        functools.partial(outer_product_kernel, sides_count * dp),
        out_shape=jax.ShapeDtypeStruct((part_rows, width), F32),
        compiler_params=pltpu.CompilerParams(vmem_limit_bytes=VMEM),
        cost_estimate=cost(4e9, 8e6),
        name="outer_product",
    )(*lows, *pairs)
    bit = 2
    while bit < seq:
        size = partial.shape[0] // 2
        high = (me[0] // bit) % 2
        keep = lax.dynamic_slice_in_dim(partial, high * size, size, axis=0)
        send = lax.dynamic_slice_in_dim(partial, (1 - high) * size, size, axis=0)
        partial = keep + swap(send.astype(BF16), bit, 0).astype(F32)
        bit *= 2
    chunk_rows = partial.shape[0]
    coded = pl.pallas_call(
        encode_kernel,
        out_shape=jax.ShapeDtypeStruct((chunk_rows + 16, width), BF16),
        cost_estimate=cost(1e7, 1e6),
        name="encode",
    )(partial)
    gathered = coded[None]
    bit = seq // 2
    while bit:
        gathered = jnp.stack([gathered, swap(gathered, bit, 0)], axis=1)
        gathered = gathered.reshape((-1,) + coded.shape)
        bit //= 2
    bits = seq.bit_length() - 1

    def place(i):
        out = 0
        for n in range(bits):
            out = out | (((i >> n) & 1) << (bits - 1 - n))
        return out

    weight_grad = pl.pallas_call(
        decode_kernel,
        grid_spec=pltpu.PrefetchScalarGridSpec(
            num_scalar_prefetch=1,
            grid=(seq,),
            in_specs=[
                pl.BlockSpec(
                    (1,) + coded.shape, lambda i, me_ref: (place(i) ^ me_ref[0], 0, 0)
                )
            ],
            out_specs=pl.BlockSpec((1, chunk_rows, width), lambda i, me_ref: (i, 0, 0)),
        ),
        out_shape=jax.ShapeDtypeStruct((seq, chunk_rows, width), F32),
        compiler_params=params(),
        cost_estimate=cost(1e7, 5e6),
        name="decode",
    )(me, gathered).reshape(own_rows, width)

    inner_specs = [
        SMEM, pair_spec, sides_spec,
        pl.BlockSpec((state, tokens), lambda i: (blocks, 0)),
        pl.BlockSpec((state, tokens), lambda i: (blocks + 1, 0)),
        heads_spec, heads_spec, column_spec, pair_spec, pair_spec,
        pl.BlockSpec((PAIR, state), lambda i: (i, 0)),
    ]
    scaled_grad, side_grad, row_sums, direct_sums = pl.pallas_call(
        inner_kernel,
        grid=(blocks,),
        in_specs=inner_specs,
        out_specs=[pair_spec, full((2 * state, tokens)), heads_spec, heads_spec],
        out_shape=[
            jax.ShapeDtypeStruct((inner, tokens), F32),
            jax.ShapeDtypeStruct((2 * state, tokens), F32),
            jax.ShapeDtypeStruct((heads, tokens), F32),
            jax.ShapeDtypeStruct((heads, tokens), F32),
        ],
        scratch_shapes=[
            pltpu.VMEM((tokens, tokens), F32),
            pltpu.VMEM((tokens, tokens), F32),
            pltpu.VMEM((state, tokens), F32),
        ],
        compiler_params=params(),
        cost_estimate=cost(1e10, 1e7),
        name="inner",
    )(
        skip_gain, features, sides, features, features, steps, cums, columns,
        scan_grad, scanned, entered,
    )

    at_pair = lambda i: (jnp.minimum(i, blocks - 1), 0)
    at_lane = lambda i: (0, i)
    input_grad, tail, returned, sums, step_grad = pl.pallas_call(
        functools.partial(outer_kernel, group),
        grid=(blocks + 2,),
        in_specs=[SMEM, SMEM]
        + [full((rows, state))] * group
        + [
            pl.BlockSpec((PAIR, tokens), at_pair),
            pl.BlockSpec((state, tokens), lambda i: (blocks, 0)),
            heads_spec,
            heads_spec,
            pl.BlockSpec((PAIR, tokens), at_pair),
            pl.BlockSpec((PAIR, tokens), at_pair),
            full((2 * state, tokens)),
            pl.BlockSpec((PAIR, state), at_pair),
            heads_spec,
            heads_spec,
            heads_spec,
            full((heads, 1)),
            full((heads, 1)),
            pl.BlockSpec((8, PAIR), lambda i: (0, jnp.minimum(i, blocks - 1))),
            pl.BlockSpec((tokens, PAIR), at_lane),
            pl.BlockSpec((tokens, PAIR), at_lane),
            pl.BlockSpec((8, PAIR), at_lane),
            pl.BlockSpec((filter_taps.shape[0], PAIR), at_lane),
        ],
        out_specs=[
            pl.BlockSpec((tokens, PAIR), at_lane),
            pl.BlockSpec((8, PAIR), at_lane),
            pl.BlockSpec((8, PAIR), at_lane),
            pl.BlockSpec((8, PAIR), at_lane),
            heads_spec,
        ],
        out_shape=[
            jax.ShapeDtypeStruct((tokens, channels), BF16),
            jax.ShapeDtypeStruct((8, channels), F32),
            jax.ShapeDtypeStruct((8, channels), F32),
            jax.ShapeDtypeStruct((8, channels), F32),
            jax.ShapeDtypeStruct((heads, tokens), F32),
        ],
        scratch_shapes=[pltpu.VMEM((state, tokens), F32)]
        + [pltpu.VMEM((heads, tokens), F32)] * 2
        + [pltpu.VMEM((heads, state), F32)],
        compiler_params=params(),
        cost_estimate=cost(3e9, 2e7),
        name="outer",
    )(
        me, skip_gain, *ending, features, features, steps, cums, scan_grad, scaled_grad,
        side_grad, entered, row_sums, direct_sums, step_rows, column(step_bias),
        column(decay_log), norm_grad, slope, raw, halo, filter_taps,
    )
    returned = lax.ppermute(returned, "seq", [(s, s - 1) for s in range(1, seq)])
    input_grad = lax.dynamic_update_slice_in_dim(
        input_grad, (tail + returned).astype(BF16), tokens - 8, axis=0
    )
    bit = 1
    while bit < dp:
        sums = sums + swap(sums, 0, bit)
        bit *= 2
    bit = 1
    while bit < seq:
        sums = sums + swap(sums, bit, 0)
        bit *= 2
    count = filter_taps.shape[0] + 1
    head_at = inner + state
    return (
        input_grad[None],
        gate_grad[None],
        step_grad[None],
        weight_grad,
        sums[:count],
        sums[count, :inner],
        sums[count : count + 3, head_at : head_at + heads],
    )


def solution(mesh):
    return jax.shard_map(
        body,
        mesh=mesh,
        in_specs=(
            P("dp", "seq", None),
            P("dp", "seq", None),
            P("dp", None, "seq"),
            P(),
            P(),
            P(),
            P(),
            P(),
            P(),
            P("dp", None),
            P("dp", "seq", None),
        ),
        out_specs=(
            P("dp", "seq", None),
            P("dp", "seq", None),
            P("dp", None, "seq"),
            P("dp", None),
            P(),
            P(),
            P(),
        ),
        check_vma=False,
    )
```

```python
import functools

import jax
import jax.numpy as jnp
from jax import lax
from jax.experimental import pallas as pl
from jax.experimental.pallas import tpu as pltpu
from jax.sharding import PartitionSpec as P

F32 = jnp.float32
BF16 = jnp.bfloat16
HIGHEST = lax.Precision.HIGHEST
MASKED = -1e30
EPSILON = 1e-05
PAIR = 128
CODE = 120.0
TINY = 1e-30
VMEM = 60 * 1024 * 1024


NN = (((1,), (0,)), ((), ()))
NT = (((1,), (1,)), ((), ()))


def cost(flops, nbytes):
    return pl.CostEstimate(flops=int(flops), bytes_accessed=int(nbytes), transcendentals=0)


def full(shape):
    zeros = (0,) * len(shape)
    return pl.BlockSpec(shape, lambda *_: zeros)


SMEM = pl.BlockSpec(memory_space=pltpu.SMEM)


def dot(a, b, dims):
    return lax.dot_general(a, b, dims, preferred_element_type=F32)


def split(x):
    high = x.astype(BF16)
    return high, (x - high.astype(F32)).astype(BF16)


def dot3(a, b, dims):
    (ah, al), (bh, bl) = a, b
    return dot(ah, bh, dims) + dot(ah, bl, dims) + dot(al, bh, dims)


def both(first, second, rows):
    width = first.shape[-1]
    return jnp.concatenate(
        [jnp.broadcast_to(first, (rows, width)), jnp.broadcast_to(second, (rows, width))], axis=0
    )


def choose(index, parts):
    out = parts[0]
    for k in range(1, len(parts)):
        out = jnp.where(index == k, parts[k], out)
    return out


def triangle(size, upper):
    row = lax.broadcasted_iota(jnp.int32, (size, size), 0)
    col = lax.broadcasted_iota(jnp.int32, (size, size), 1)
    return row <= col if upper else row >= col


def call(kernel, args, in_specs, out_shape, out_specs, grid=(1,), after=(), scratch=(), name=None,
         flops=1e8, nbytes=1e6):
    count, extra = len(args), len(after)

    def run(*refs):
        kernel(*refs[:count], *refs[count + extra :])

    return pl.pallas_call(
        run,
        grid=grid,
        in_specs=list(in_specs) + [pl.BlockSpec(memory_space=pl.ANY)] * extra,
        out_specs=out_specs,
        out_shape=out_shape,
        scratch_shapes=list(scratch),
        compiler_params=pltpu.CompilerParams(
            dimension_semantics=("arbitrary",) * len(grid), vmem_limit_bytes=VMEM
        ),
        cost_estimate=cost(flops, nbytes),
        name=name,
    )(*args, *after)


def shaped(shape, dtype=F32):
    return jax.ShapeDtypeStruct(shape, dtype)


def steps_kernel(step_ref, bias_ref, log_ref, steps_ref, cums_ref, columns_ref):
    raw = step_ref[...] + bias_ref[...]
    steps = jnp.maximum(raw, 0.0) + jnp.log1p(jnp.exp(-jnp.abs(raw)))
    rates = -jnp.exp(log_ref[...]) * steps
    heads, size = raw.shape
    ones = jnp.where(triangle(size, True), 1.0, 0.0).astype(F32)
    cums = lax.dot_general(rates, ones, NN, precision=HIGHEST, preferred_element_type=F32)
    steps_ref[...] = steps
    cums_ref[...] = cums
    columns_ref[...] = jnp.concatenate([cums, jnp.zeros((PAIR - heads, size), F32)], axis=0).T


def extend(halo, raw):
    return jnp.concatenate([halo.astype(F32), raw.astype(F32)], axis=0)


def activation(extended, taps, bias):
    width = taps.shape[0]
    start = 8 - width + 1
    size = extended.shape[0] - 8
    filtered = bias + taps[0:1] * extended[start : start + size]
    for k in range(1, width):
        filtered = filtered + taps[k : k + 1] * extended[start + k : start + k + size]
    gate = jax.nn.sigmoid(filtered)
    active = filtered * gate
    return active, gate + active * (1.0 - gate)


def filter_kernel(
    me_ref, halo_ref, raw_ref, taps_ref, bias_ref,
    side_halo_ref, side_raw_ref, side_taps_ref, side_bias_ref, steps_ref, cums_ref,
    slope_ref, features_ref, side_slope_ref, side_features_ref, sides_ref, *rest,
):
    chunks, (key_high, key_low) = rest[:-2], rest[-2:]
    i = pl.program_id(0)
    size, lanes = raw_ref.shape
    units = lanes // PAIR
    extra = 16

    @pl.when(i == 0)
    def _():
        for u in range(side_raw_ref.shape[1] // PAIR):
            at = slice(u * PAIR, (u + 1) * PAIR)
            active, slope = activation(
                extend(side_halo_ref[:, at], side_raw_ref[:, at]), side_taps_ref[:, at],
                side_bias_ref[:, at],
            )
            side_slope_ref[:, at] = slope
            side_features_ref[at, :] = active.T
            sides_ref[:, at] = active
            if u == 0:
                key_high[...], key_low[...] = split(active)

    slot = i ^ (me_ref[0] % len(chunks))
    keys = (key_high[...], key_low[...])
    lasts = []
    states = []
    for u in range(units):
        at = slice(u * PAIR, (u + 1) * PAIR)
        active, slope = activation(
            extend(halo_ref[:, at], raw_ref[:, at]), taps_ref[:, at], bias_ref[:, at]
        )
        slope_ref[:, at] = slope
        features = active.T
        features_ref[at, :] = features
        rows = []
        for j in range(2):
            head = (i * units + u) * 2 + j
            cums = cums_ref[pl.ds(head, 1), :]
            last = cums[:, size - 1 :]
            lasts.append(jnp.broadcast_to(jnp.exp(last), (1, PAIR)))
            rows.append(steps_ref[pl.ds(head, 1), :] * jnp.exp(last - cums))
        scaled = features * both(rows[0], rows[1], PAIR // 2)
        states.append(dot3(split(scaled), keys, NN).astype(BF16))
    lasts.append(jnp.zeros((extra - len(lasts), PAIR), F32))
    decay_high, decay_low = split(jnp.concatenate(lasts, axis=0))
    for k, chunk in enumerate(chunks):

        @pl.when(slot == k)
        def _():
            for u in range(units):
                chunk[u * PAIR : (u + 1) * PAIR, :] = states[u]
            chunk[lanes : lanes + extra, :] = decay_high
            chunk[lanes + extra :, :] = decay_low


def scan_chunk(group, reverse, width, me_ref, decays, parts, carry_ref, scratch, total_ref):
    here = me_ref[0] % group
    rows_all = total_ref.shape[0] if total_ref is not None else carry_ref.shape[0]
    order = range(group - 1, -1, -1) if reverse else range(group)
    fall = [
        choose(here ^ p, [d[:16, :].astype(F32) + d[16:, :].astype(F32) for d in decays])
        for p in range(group)
    ]
    for h in range(rows_all // width):
        rows = pl.ds(h * width, width)
        if carry_ref is None:
            running = jnp.zeros((width, parts[0].shape[1]), F32)
        else:
            running = carry_ref[rows, :].astype(F32)
        for n, p in enumerate(order):
            if scratch is not None:
                scratch[p, rows, :] = running
                if n == group - 1:
                    break
            term = choose(here ^ p, [part[rows, :] for part in parts]).astype(F32)
            running = term + fall[p][h : h + 1, :] * running
        if total_ref is not None:
            total_ref[rows, :] = running.astype(BF16)


def carry_kernel(group, reverse, width, me_ref, *refs):
    decays, parts, out_ref = refs[:group], refs[group : 2 * group], refs[2 * group]
    scan_chunk(group, reverse, width, me_ref, decays, parts, None, None, out_ref)


def spread_kernel(group, reverse, width, me_ref, *refs):
    decays, parts, carry_ref = refs[:group], refs[group : 2 * group], refs[2 * group]
    outs, scratch = refs[2 * group + 1 : 3 * group + 1], refs[3 * group + 1]
    scan_chunk(group, reverse, width, me_ref, decays, parts, carry_ref, scratch, None)
    here = me_ref[0] % group
    for k in range(group):
        outs[k][...] = scratch[here ^ k].astype(BF16)


class Exchange:
    def __init__(self, me, seq, group, rows, state, head_dim, reverse):
        self.me, self.seq, self.group, self.reverse = me, seq, group, reverse
        self.rows, self.state, self.head_dim = rows, state, head_dim

    def swap(self, value, k):
        return lax.ppermute(value, "seq", [(s, s ^ k) for s in range(self.seq)])

    def send(self, chunks):
        self.got = [chunks[0]] + [self.swap(chunks[k], k) for k in range(1, self.group)]

    def specs(self, decays):
        row = self.rows // 32
        return (
            [SMEM]
            + [pl.BlockSpec((32, self.state), lambda i: (row, 0))] * self.group
            + [pl.BlockSpec((self.rows, self.state), lambda i: (0, 0))] * self.group
        )

    def total(self, decays, after=()):
        self.decays = decays
        groups = self.seq // self.group
        shape = (self.rows, self.state)
        total = call(
            functools.partial(carry_kernel, self.group, self.reverse, self.head_dim),
            [self.me, *decays, *self.got], self.specs(decays), shaped(shape, BF16), full(shape),
            after=after, name="scan_total",
        )
        g = self.group
        ways = (
            [(s, s - g) for s in range(g, self.seq)]
            if self.reverse
            else [(s, s + g) for s in range(self.seq - g)]
        )
        carry = lax.ppermute(total, "seq", ways)
        if groups > 2:
            product = 1.0
            for d in decays:
                tail = d[self.rows :].astype(F32)
                product = product * (tail[:16] + tail[16:])
            product = jnp.repeat(product[: self.rows // self.head_dim], self.head_dim, axis=0)
            for _ in range(groups - 2):
                step = total.astype(F32) + product * carry.astype(F32)
                carry = lax.ppermute(step.astype(BF16), "seq", ways)
        self.carry = carry
        return total

    def spread(self, after=()):
        shape = (self.rows, self.state)
        g = self.group
        self.outs = call(
            functools.partial(spread_kernel, g, self.reverse, self.head_dim),
            [self.me, *self.decays, *self.got, self.carry],
            self.specs(self.decays) + [full(shape)],
            [shaped(shape, BF16)] * g, [full(shape)] * g, after=after,
            scratch=[pltpu.VMEM((g,) + shape, F32)], name="scan_spread",
        )
        return [self.outs[0]] + [self.swap(self.outs[k], k) for k in range(1, g)]


def column_of(columns_ref, first):
    return pltpu.roll(columns_ref[...], PAIR - first, 1)


def falls(row, column, half, low):
    first = jnp.exp(jnp.where(low[0], row - column[:half], MASKED))
    second = jnp.exp(jnp.where(low[1], row[:, half:] - column[half:], MASKED))
    return first, second


def masks(size):
    half = size // 2
    row = lax.broadcasted_iota(jnp.int32, (half, size), 0)
    col = lax.broadcasted_iota(jnp.int32, (half, size), 1)
    return row <= col, triangle(half, True)


def scores(sides_ref, score_ref):
    sides = sides_ref[...]
    state = sides.shape[1] // 2
    score_ref[...] = dot3(split(sides[:, :state]), split(sides[:, state:]), NT)


def pad_left(value, size):
    return jnp.concatenate([jnp.zeros((value.shape[0], size), F32), value], axis=1)


def inside_kernel(
    first_head, skip_ref, features_ref, sides_ref, steps_ref, cums_ref, columns_ref,
    out_ref, score_ref,
):
    i = pl.program_id(0)

    @pl.when(i == 0)
    def _():
        scores(sides_ref, score_ref)

    size = score_ref.shape[0]
    low = masks(size)
    span = PAIR // 2
    half = size // 2
    units = out_ref.shape[0] // span
    base = first_head + i * units
    columns = column_of(columns_ref, base)
    for j in range(units):
        part = slice(j * span, (j + 1) * span)
        values = features_ref[part, :]
        scaled = values * steps_ref[pl.ds(base + j, 1), :]
        fall = falls(cums_ref[pl.ds(base + j, 1), :], columns[:, j : j + 1], half, low)
        ah, al = split(score_ref[:half, :] * fall[0])
        bh, bl = split(score_ref[half:, half:] * fall[1])
        xh, xl = split(scaled)
        stack = jnp.concatenate([xh, xl], axis=0)
        first = dot(stack[:, :half], ah, NN)
        second = dot(stack[:, half:], bh, NN)
        inside = first[:span] + first[span:] + dot(xh[:, :half], al, NN)
        later = second[:span] + second[span:] + dot(xh[:, half:], bl, NN)
        inside = inside + pad_left(later, half)
        out_ref[part, :] = inside + skip_ref[base + j] * values


def inner_kernel(
    first_head, skip_ref, features_ref, sides_ref, steps_ref, cums_ref, columns_ref,
    cotangent_ref, scanned_ref, entering_ref, *refs
):
    if len(refs) == 9:
        total_in, carried_in, refs = refs[0], refs[1], refs[2:]
    else:
        total_in = carried_in = None
    grad_ref, row_ref, direct_ref, total_out, carried_out, score_ref, total_ref = refs
    i = pl.program_id(0)

    @pl.when(i == 0)
    def _():
        scores(sides_ref, score_ref)
        if total_in is None:
            total_ref[...] = jnp.zeros_like(total_ref)
            carried_out[...] = jnp.zeros_like(carried_out)
        else:
            total_ref[...] = total_in[...]
            carried_out[...] = carried_in[...]

    size = score_ref.shape[0]
    low = masks(size)
    span = PAIR // 2
    half = size // 2
    units = grad_ref.shape[0] // span
    base = first_head + i * units
    columns = column_of(columns_ref, base)
    decayed = []
    for j in range(units):
        part = slice(j * span, (j + 1) * span)
        values = features_ref[part, :]
        cotangent = cotangent_ref[part, :]
        scaled = values * steps_ref[pl.ds(base + j, 1), :]
        row = cums_ref[pl.ds(base + j, 1), :]
        fall = falls(row, columns[:, j : j + 1], half, low)
        ah, al = split(score_ref[:half, :] * fall[0])
        bh, bl = split(score_ref[half:, half:] * fall[1])
        gh, gl = split(cotangent)
        xh, xl = split(scaled.T)
        stack = jnp.concatenate([gh, gl], axis=0)
        first = dot(stack, ah, NT)
        second = dot(stack[:, half:], bh, NT)
        grad_ref[part, :half] = first[:span] + first[span:] + dot(gh, al, NT)
        grad_ref[part, half:] = second[:span] + second[span:] + dot(gh[:, half:], bl, NT)
        left = jnp.concatenate([xh, xh, xl], axis=1)
        right = jnp.concatenate([gh, gl, gh], axis=0)
        total_ref[:half, :] += dot(left[:half], right, NN) * fall[0]
        total_ref[half:, half:] += dot(left[half:], right[:, half:], NN) * fall[1]
        direct = cotangent * values
        skip = skip_ref[base + j]
        here = i * units + j
        row_ref[pl.ds(here, 1), :] = jnp.sum(
            cotangent * scanned_ref[part, :] - skip * direct, axis=0, keepdims=True
        )
        direct_ref[pl.ds(here, 1), :] = jnp.sum(direct, axis=0, keepdims=True)
        decayed.append(cotangent * jnp.exp(row))
    ch, cl = split(jnp.concatenate(decayed, axis=0))
    entering = entering_ref[...].astype(F32).T.astype(BF16)
    carried_out[...] += dot(entering, ch, NN) + dot(entering, cl, NN)

    @pl.when(i == pl.num_programs(0) - 1)
    def _():
        total_out[...] = total_ref[...]


def norm_kernel(group, dp, halves, me_ref, *refs):
    states, refs = refs[:group], refs[group:]
    grads, refs = refs[:dp], refs[dp:]
    (local_a, local_b, gate_ref, cums_ref, sides_ref, query_ref, weight_ref), refs = refs[:7], refs[7:]
    (scanned_ref, cotangent_ref, gate_grad_ref, norm_ref, entering_ref), refs = refs[:5], refs[5:]
    entries, refs = refs[:group], refs[group:]
    lows, refs = refs[: halves * dp], refs[halves * dp :]
    gated_s, open_s, slope_s, grad_s, square_s, cross_s = refs
    phase, b = pl.program_id(0), pl.program_id(1)
    lanes = gate_ref.shape[1]
    units = lanes // PAIR
    half = PAIR // 2
    size = local_a.shape[1]
    blocks = pl.num_programs(1)

    def exps(u):
        head = (b * units + u) * 2
        return both(
            jnp.exp(cums_ref[pl.ds(head, 1), :]), jnp.exp(cums_ref[pl.ds(head + 1, 1), :]), half
        )

    @pl.when(phase == 0)
    def _():
        queries = split(query_ref[...])
        slot = (me_ref[0] % group) ^ b
        source = me_ref[1] ^ b
        scale = choose(source, [g[lanes : lanes + 1, :] for g in grads]).astype(F32) * (1.0 / CODE)
        square = cross = 0.0
        for u in range(units):
            at = slice(u * PAIR, (u + 1) * PAIR)
            here = pl.ds(b * lanes + u * PAIR, PAIR)
            entering = choose(slot, [s[at, :] for s in states])
            entering_ref[at, :] = entering
            carried = dot(entering, queries[0], NN) + dot(entering, queries[1], NN)
            local = jnp.where(b < blocks // 2, local_a[at, :], local_b[at, :])
            scanned = local + carried * exps(u)
            scanned_ref[at, :] = scanned
            z = gate_ref[:, at].astype(F32).T
            opened = jax.nn.sigmoid(z)
            through = z * opened
            gated = scanned * through
            grad = jnp.log2(choose(source, [g[at, :] for g in grads]).astype(F32)) * scale
            gated_s[here, :] = gated
            open_s[here, :] = through
            slope_s[here, :] = scanned * (opened + through * (1.0 - opened))
            grad_s[here, :] = grad
            square = square + jnp.sum(gated * gated, axis=0, keepdims=True)
            cross = cross + jnp.sum(gated * (grad * weight_ref[at, :]), axis=0, keepdims=True)

        @pl.when(b == 0)
        def _():
            square_s[...] = square
            cross_s[...] = cross

        @pl.when(b > 0)
        def _():
            square_s[...] += square
            cross_s[...] += cross

    @pl.when(phase == 1)
    def _():
        share = 1.0 / (blocks * lanes)
        inverse = lax.rsqrt(square_s[...] * share + EPSILON)
        shift = inverse * inverse * inverse * (cross_s[...] * share)
        sides = split(sides_ref[...])
        ones = jnp.ones((8, size), BF16)
        results, heads = [], []
        for u in range(units):
            at = slice(u * PAIR, (u + 1) * PAIR)
            here = pl.ds(b * lanes + u * PAIR, PAIR)
            gated, grad, weight = gated_s[here, :], grad_s[here, :], weight_ref[at, :]
            unit = gated * inverse
            results.append((unit * weight).astype(BF16))
            product = split(unit * grad)
            norm_ref[:, at] = dot(ones, product[0], NT) + dot(ones, product[1], NT)
            gated_grad = inverse * (grad * weight) - gated * shift
            cotangent = gated_grad * open_s[here, :]
            cotangent_ref[at, :] = cotangent
            gate_grad_ref[:, at] = (gated_grad * slope_s[here, :]).T.astype(BF16)
            heads.append(dot3(split(cotangent * exps(u)), sides, NN).astype(BF16))
        entry = (me_ref[0] % group) ^ b
        for k in range(group):

            @pl.when(entry == k)
            def _():
                for u in range(units):
                    entries[k][u * PAIR : (u + 1) * PAIR, :] = heads[u]

        low = jnp.concatenate(results, axis=0)
        part = lanes // halves
        for ks in range(halves):
            for kd in range(dp):
                for n in range(halves):

                    @pl.when(((me_ref[1] ^ b) == kd) & ((n ^ (me_ref[0] % halves)) == ks))
                    def _():
                        lows[ks * dp + kd][...] = low[n * part : (n + 1) * part]


def outer_kernel(group, me_ref, skip_ref, *refs):
    states, refs = refs[:group], refs[group:]
    (
        features_ref, side_features_ref, steps_ref, cums_ref, cotangent_ref, grad_a, grad_b,
        total_ref, carried_ref, entering_ref, row_a, row_b, direct_a, direct_b, step_in_ref,
        bias_ref, log_ref, norm_ref, slope_ref, raw_ref, halo_ref, taps_ref,
        side_slope_ref, side_raw_ref, side_halo_ref, side_taps_ref,
        out_ref, tail_ref, back_ref, sums_ref, step_ref,
        key_grad_s, value_s, end_s, decay_s,
    ) = refs
    i = pl.program_id(0)
    blocks = pl.num_programs(0) - 1
    half = PAIR // 2
    size, lanes = raw_ref.shape
    units = lanes // PAIR
    heads = steps_ref.shape[0]
    state = side_features_ref.shape[0] // 2

    @pl.when(i == 0)
    def _():
        key_grad_s[...] = jnp.zeros_like(key_grad_s)

    def filtered(grad, slope, halo, raw, taps, at):
        df = grad.T * slope
        width = taps.shape[0]
        longer = jnp.concatenate([df, jnp.zeros((8, PAIR), F32)], axis=0)
        ahead = jnp.concatenate([jnp.zeros((8, PAIR), F32), df[0:8]], axis=0)
        extended = extend(halo, raw)
        start = 8 - width + 1
        last = width - 1
        own = taps[0:1] * longer[last : last + size]
        back = taps[0:1] * ahead[last : last + 8]
        sums = [jnp.sum(df * extended[start : start + size], axis=0, keepdims=True)]
        for k in range(1, width):
            own = own + taps[k : k + 1] * longer[last - k : last - k + size]
            back = back + taps[k : k + 1] * ahead[last - k : last - k + 8]
            sums.append(
                jnp.sum(df * extended[start + k : start + k + size], axis=0, keepdims=True)
            )
        sums.append(jnp.sum(df, axis=0, keepdims=True))
        out_ref[:, at] = own.astype(BF16)
        tail_ref[:, at] = own[size - 8 :]
        back_ref[:, at] = back
        return sums

    @pl.when(i < blocks)
    def _():
        b = jnp.minimum(i, blocks - 1)
        slot = (me_ref[0] % group) ^ b
        keys = split(side_features_ref[:state, :])
        total = 0.0
        for u in range(units):
            at = slice(u * PAIR, (u + 1) * PAIR)
            ending = choose(slot, [s[at, :] for s in states])
            from_end = dot(ending, keys[0], NN) + dot(ending, keys[1], NN)
            tops, steps = [], []
            first = (b * units + u) * 2
            for j in range(2):
                cums = cums_ref[pl.ds(first + j, 1), :]
                tops.append(jnp.exp(cums[:, size - 1 :] - cums))
                steps.append(steps_ref[pl.ds(first + j, 1), :])
            top = both(tops[0], tops[1], half)
            step = both(steps[0], steps[1], half)
            values = features_ref[at, :]
            from_end = from_end * top
            grad = jnp.where(b < blocks // 2, grad_a[at, :], grad_b[at, :]) + from_end
            scaled = values * step
            sh, sl = split(scaled * top)
            ends = ending.astype(F32)
            turned = ends.T.astype(BF16)
            total = total + dot(turned, sh, NN) + dot(turned, sl, NN)
            by_value = values * grad
            by_end = scaled * from_end
            product = ends * entering_ref[at, :].astype(F32)
            skips = []
            for j in range(2):
                part = slice(j * half, (j + 1) * half)
                row = pl.ds(first + j, 1)
                value_s[row, :] = jnp.sum(by_value[part], axis=0, keepdims=True)
                end_s[row, :] = jnp.sum(by_end[part], axis=0, keepdims=True)
                decay_s[row, :] = jnp.sum(product[part], axis=0, keepdims=True)
                skips.append(
                    skip_ref[first + j]
                    * cotangent_ref[u * PAIR + j * half : u * PAIR + (j + 1) * half, :]
                )
            where = pl.ds(pl.multiple_of(b * lanes + u * PAIR, PAIR), PAIR)
            sums = filtered(
                jnp.concatenate(skips, axis=0) + grad * step, slope_ref[:, at], halo_ref[:, at],
                raw_ref[:, at], taps_ref[:, at], where,
            )
            sums.append(norm_ref[0:1, at])
            sums_ref[:, where] = jnp.concatenate(
                sums + [jnp.zeros((8 - len(sums), PAIR), F32)], axis=0
            )
        key_grad_s[...] += total

    @pl.when(i == blocks)
    def _():
        score = split(total_ref[...])
        inner = blocks * lanes
        steps, cums = steps_ref[...], cums_ref[...]
        values = value_s[...]
        rows = jnp.concatenate([row_a[...], row_b[...]], axis=0)
        direct = jnp.concatenate([direct_a[...], direct_b[...]], axis=0)
        base = rows - steps * values
        ones = jnp.where(triangle(size, False), 1.0, 0.0).astype(F32)
        rate_grad = lax.dot_general(base, ones, NN, precision=HIGHEST, preferred_element_type=F32)
        ended = jnp.sum(end_s[...], axis=1, keepdims=True)
        kept = jnp.exp(cums[:, size - 1 :]) * jnp.sum(decay_s[...], axis=1, keepdims=True)
        rate_grad = rate_grad + (ended + kept)
        rate = -jnp.exp(log_ref[...])
        step_grad = (values + rate_grad * rate) * jax.nn.sigmoid(step_in_ref[...] + bias_ref[...])
        step_ref[...] = step_grad
        row = lax.broadcasted_iota(jnp.int32, (heads, PAIR), 0)
        col = lax.broadcasted_iota(jnp.int32, (heads, PAIR), 1)
        head_rows = []
        for source in (step_grad, rate_grad * steps * rate, direct):
            column = jnp.sum(source, axis=1, keepdims=True)
            head_rows.append(jnp.sum(jnp.where(row == col, column, 0.0), axis=0, keepdims=True))
        keys = side_features_ref[:state, :]
        queries = side_features_ref[state:, :]
        key_grad = dot3(split(queries), score, NT) + key_grad_s[...]
        query_grad = dot3(split(keys), score, NN) + carried_ref[...]
        for u, grad in enumerate((key_grad, query_grad)):
            at = slice(u * PAIR, (u + 1) * PAIR)
            where = slice(inner + u * PAIR, inner + (u + 1) * PAIR)
            sums = filtered(
                grad, side_slope_ref[:, at], side_halo_ref[:, at], side_raw_ref[:, at],
                side_taps_ref[:, at], where,
            )
            sums_ref[:, where] = jnp.concatenate(sums + head_rows, axis=0)


def encode(values):
    scale = jnp.max(jnp.abs(values), axis=0, keepdims=True) * 1.01 + TINY
    scale = scale.astype(BF16)
    coded = jnp.exp2(values * (CODE / scale.astype(F32))).astype(BF16)
    return coded, jnp.broadcast_to(scale, (16, values.shape[1]))


def project_kernel(count, weight_ref, *refs):
    cotangents, outs = refs[:count], refs[count:]
    rows = weight_ref.shape[0]
    for k in range(count):
        coded, scale = encode(dot(weight_ref[...], cotangents[k][...], NT))
        outs[k][:rows, :] = coded
        outs[k][rows:, :] = scale


def outer_product_kernel(count, peers, me_ref, *refs):
    lows, cotangents, keep_ref = refs[:count], refs[count : 2 * count], refs[2 * count]
    sends = refs[2 * count + 1 :]
    total = dot(lows[0][...], cotangents[0][...], NN)
    for k in range(1, count):
        total = total + dot(lows[k][...], cotangents[k][...], NN)
    rows = keep_ref.shape[0]
    here = me_ref[0] // 2
    for p in range(peers):
        piece = total[p * rows : (p + 1) * rows]

        @pl.when(here == p)
        def _():
            keep_ref[...] = piece

        for k in range(1, peers):

            @pl.when((here ^ k) == p)
            def _():
                sends[k - 1][...] = piece.astype(BF16)


def fold_kernel(keep_ref, *refs):
    parts, out_ref = refs[:-1], refs[-1]
    values = keep_ref[...]
    for part in parts:
        values = values + part[...].astype(F32)
    coded, scale = encode(values)
    rows = keep_ref.shape[0]
    out_ref[:rows, :] = coded
    out_ref[rows:, :] = scale


def decode_kernel(peers, me_ref, *refs):
    parts, out_ref = refs[:peers], refs[-1]
    rows = out_ref.shape[0] // peers
    here = me_ref[0] // 2
    for p in range(peers):
        coded = choose(here ^ p, [part[...] for part in parts])
        scale = coded[rows : rows + 1, :].astype(F32) * (1.0 / CODE)
        out_ref[p * rows : (p + 1) * rows, :] = jnp.log2(coded[:rows, :].astype(F32)) * scale


def body(
    conv_input, gate_input, step_input, filter_taps, filter_bias, step_bias, decay_log,
    skip_gain, norm_weight, output_weight, output_grad,
):
    seq, dp = lax.axis_size("seq"), lax.axis_size("dp")
    me = jnp.stack([lax.axis_index("seq"), lax.axis_index("dp")]).astype(jnp.int32)
    group = dp
    raw, gate, step_rows, cotangent = conv_input[0], gate_input[0], step_input[0], output_grad[0]
    tokens, channels = raw.shape
    inner = gate.shape[1]
    heads = step_rows.shape[0]
    head_dim = inner // heads
    state = (channels - inner) // 2
    width = cotangent.shape[1]
    taps_count = filter_taps.shape[0]
    rows = inner // group
    side = 2 * state
    both_axes = ("seq", "dp")

    def swap(value, seq_bits, dp_bits):
        pairs = [
            (s * dp + d, (s ^ seq_bits) * dp + (d ^ dp_bits)) for s in range(seq) for d in range(dp)
        ]
        return lax.ppermute(value, both_axes, pairs)

    halo = lax.ppermute(raw[-8:], "seq", [(s, s + 1) for s in range(seq - 1)])

    known = {(0, 0): cotangent}
    bit = dp // 2
    while bit:
        for key in list(known):
            known[(0, key[1] | bit)] = swap(known[key], 0, bit)
        bit //= 2

    column = lambda v: v.reshape(-1, 1)
    heads_shape = (heads, tokens)
    step_bias, decay_log = column(step_bias), column(decay_log)
    steps, cums, columns = call(
        steps_kernel, [step_rows, step_bias, decay_log],
        [full(heads_shape), full((heads, 1)), full((heads, 1))],
        [shaped(heads_shape), shaped(heads_shape), shaped((tokens, PAIR))],
        [full(heads_shape), full(heads_shape), full((tokens, PAIR))],
        name="steps",
    )

    at_chunk = lambda i: (0, i)
    at_side = lambda i: (0, inner // side)
    bias_row = filter_bias.reshape(1, -1)
    payload = (rows + 32, state)
    slope, features, side_slope, side_features, sides, *chunks = call(
        filter_kernel,
        [me, halo, raw, filter_taps, bias_row, halo, raw, filter_taps, bias_row, steps, cums],
        [SMEM]
        + [pl.BlockSpec((n, rows), at_chunk) for n in (8, tokens, taps_count, 1)]
        + [pl.BlockSpec((n, side), at_side) for n in (8, tokens, taps_count, 1)]
        + [full(heads_shape)] * 2,
        [
            shaped((tokens, inner)), shaped((inner, tokens)), shaped((tokens, side)),
            shaped((side, tokens)), shaped((tokens, side)),
        ]
        + [shaped(payload, BF16)] * group,
        [
            pl.BlockSpec((tokens, rows), at_chunk), pl.BlockSpec((rows, tokens), lambda i: (i, 0)),
            full((tokens, side)), full((side, tokens)), full((tokens, side)),
        ]
        + [full(payload)] * group,
        grid=(group,), scratch=[pltpu.VMEM((tokens, state), BF16)] * 2, name="filter",
        flops=1e9, nbytes=1e7,
    )

    forward = Exchange(me, seq, group, rows, state, head_dim, False)
    forward.send(chunks)
    decays = forward.got

    units = 2 * PAIR
    parts = inner // units // 2
    pair_shape = (units, tokens)

    def inside(n, after):
        return call(
            functools.partial(inside_kernel, n * heads // 2),
            [skip_gain, features, sides, steps, cums, columns],
            [
                SMEM, pl.BlockSpec(pair_shape, lambda i: (n * parts + i, 0)), full((tokens, side)),
                full(heads_shape), full(heads_shape), full((tokens, PAIR)),
            ],
            shaped((inner // 2, tokens)), pl.BlockSpec(pair_shape, lambda i: (i, 0)),
            grid=(parts,), after=after, scratch=[pltpu.VMEM((tokens, tokens), F32)],
            name="inside", flops=4e9, nbytes=3e6,
        )

    local_a = inside(0, ())
    total = forward.total(decays, (local_a,))

    piece = (rows + 16, tokens)
    served = call(
        functools.partial(project_kernel, dp),
        [output_weight] + [known[(0, k)] for k in range(dp)],
        [full((rows, width))] + [full((tokens, width))] * dp,
        [shaped(piece, BF16)] * dp, [full(piece)] * dp, after=(total,),
        name="project", flops=4e9, nbytes=8e6,
    )
    grads = [served[0]] + [swap(served[k], 0, k) for k in range(1, dp)]
    entering = forward.spread((served[0],))
    local_b = inside(1, (forward.outs[0],))

    halves = 2
    for k in range(dp):
        if k % 2 == 0:
            known[(1, k)] = swap(known[(0, k)], 1, 0)
    for k in range(dp):
        if k % 2 == 1:
            known[(1, k)] = swap(known[(1, k - 1)], 0, 1)

    entry_shape, low_shape = (rows, state), (rows // halves, tokens)
    norm_out = lambda p, b: jnp.where(p == 1, b, 0)
    norm_in = lambda p, b: jnp.where(p == 0, b, group - 1)
    scanned, scan_grad, gate_grad, norm_grad, entered, *rest = call(
        functools.partial(norm_kernel, group, dp, halves),
        [me, *entering, *grads, local_a, local_b, gate, cums, sides, side_features,
         column(norm_weight)],
        [SMEM] + [full(entry_shape)] * group + [full(piece)] * dp
        + [
            pl.BlockSpec((rows, tokens), lambda p, b: (jnp.minimum(norm_in(p, b), group // 2 - 1), 0)),
            pl.BlockSpec((rows, tokens), lambda p, b: (jnp.maximum(norm_in(p, b) - group // 2, 0), 0)),
            pl.BlockSpec((tokens, rows), lambda p, b: (0, norm_in(p, b))),
            full(heads_shape),
            pl.BlockSpec((tokens, state), lambda p, b: (0, 1)),
            pl.BlockSpec((state, tokens), lambda p, b: (1, 0)),
            pl.BlockSpec((rows, 1), lambda p, b: (b, 0)),
        ],
        [
            shaped((inner, tokens)), shaped((inner, tokens)), shaped((tokens, inner), BF16),
            shaped((8, inner)), shaped((inner, state), BF16),
        ]
        + [shaped(entry_shape, BF16)] * group
        + [shaped(low_shape, BF16)] * (halves * dp),
        [
            pl.BlockSpec((rows, tokens), lambda p, b: (norm_in(p, b), 0)),
            pl.BlockSpec((rows, tokens), lambda p, b: (norm_out(p, b), 0)),
            pl.BlockSpec((tokens, rows), lambda p, b: (0, norm_out(p, b))),
            pl.BlockSpec((8, rows), lambda p, b: (0, norm_out(p, b))),
            pl.BlockSpec((rows, state), lambda p, b: (norm_in(p, b), 0)),
        ]
        + [full(entry_shape)] * group
        + [full(low_shape)] * (halves * dp),
        grid=(2, group),
        scratch=[pltpu.VMEM((inner, tokens), F32)] * 4 + [pltpu.VMEM((1, tokens), F32)] * 2,
        name="norm", flops=3e9, nbytes=2e7,
    )
    entries, lows = rest[:group], rest[group:]

    sent = [
        low if n == 0 else swap(low, n // dp, n % dp) for n, low in enumerate(lows)
    ]
    backward = Exchange(me, seq, group, rows, state, head_dim, True)
    backward.send(entries)

    def inner_call(n, before, after):
        half_heads = (heads // 2, tokens)
        specs = [
            SMEM, pl.BlockSpec(pair_shape, lambda i: (n * parts + i, 0)), full((tokens, side)),
            full(heads_shape), full(heads_shape), full((tokens, PAIR)),
            pl.BlockSpec(pair_shape, lambda i: (n * parts + i, 0)),
            pl.BlockSpec(pair_shape, lambda i: (n * parts + i, 0)),
            pl.BlockSpec((units, state), lambda i: (n * parts + i, 0)),
        ] + [full((tokens, tokens)), full((state, tokens))][: len(before)]
        return call(
            functools.partial(inner_kernel, n * heads // 2),
            [skip_gain, features, sides, steps, cums, columns, scan_grad, scanned, entered, *before],
            specs,
            [
                shaped((inner // 2, tokens)), shaped(half_heads), shaped(half_heads),
                shaped((tokens, tokens)), shaped((state, tokens)),
            ],
            [
                pl.BlockSpec(pair_shape, lambda i: (i, 0)), full(half_heads), full(half_heads),
                full((tokens, tokens)), full((state, tokens)),
            ],
            grid=(parts,), after=after, scratch=[pltpu.VMEM((tokens, tokens), F32)] * 2,
            name="inner", flops=5e9, nbytes=5e6,
        )

    grad_a, row_a, direct_a, total_a, carried_a = inner_call(0, (), ())
    total = backward.total(decays, (grad_a,))

    peers = seq // halves
    count = halves * dp
    part_rows = rows // halves // peers
    keep, *sends = call(
        functools.partial(outer_product_kernel, count, peers),
        [me, *sent] + [known[(n // dp, n % dp)] for n in range(count)],
        [SMEM] + [full(low_shape)] * count + [full((tokens, width))] * count,
        [shaped((part_rows, width))] + [shaped((part_rows, width), BF16)] * (peers - 1),
        [full((part_rows, width))] * peers, after=(total,),
        name="outer_product", flops=4e9, nbytes=8e6,
    )
    arrived = [swap(sends[k - 1], halves * k, 0) for k in range(1, peers)]
    ending = backward.spread((keep,))
    grad_b, row_b, direct_b, total_b, carried_b = inner_call(
        1, (total_a, carried_a), (backward.outs[0],)
    )

    coded_shape = (part_rows + 16, width)
    coded = call(
        fold_kernel, [keep, *arrived], [full((part_rows, width))] * peers,
        shaped(coded_shape, BF16), full(coded_shape), after=(grad_b,), name="fold",
    )
    gathered = [coded] + [swap(coded, halves * k, 0) for k in range(1, peers)]

    last = lambda i: jnp.minimum(i, group - 1)
    chunk_rows = lambda i: (last(i), 0)
    chunk_lanes = lambda i: (0, last(i))
    half_heads = (heads // 2, tokens)
    wide = lambda n: full((n, channels))
    input_grad, tail, returned, sums, step_grad = call(
        functools.partial(outer_kernel, group),
        [
            me, skip_gain, *ending, features, side_features, steps, cums, scan_grad, grad_a, grad_b,
            total_b, carried_b, entered, row_a, row_b, direct_a, direct_b, step_rows, step_bias,
            decay_log, norm_grad, slope, raw, halo, filter_taps, side_slope, raw, halo, filter_taps,
        ],
        [SMEM, SMEM] + [full(entry_shape)] * group
        + [
            pl.BlockSpec((rows, tokens), chunk_rows), full((side, tokens)),
            full(heads_shape), full(heads_shape),
            pl.BlockSpec((rows, tokens), chunk_rows),
            pl.BlockSpec((rows, tokens), lambda i: (jnp.minimum(i, group // 2 - 1), 0)),
            pl.BlockSpec((rows, tokens), lambda i: (jnp.maximum(last(i) - group // 2, 0), 0)),
            full((tokens, tokens)), full((state, tokens)),
            pl.BlockSpec((rows, state), chunk_rows),
            full(half_heads), full(half_heads), full(half_heads), full(half_heads),
            full(heads_shape), full((heads, 1)), full((heads, 1)),
        ]
        + [pl.BlockSpec((n, rows), chunk_lanes) for n in (8, tokens, tokens, 8, taps_count)]
        + [full((tokens, side))]
        + [pl.BlockSpec((n, side), at_side) for n in (tokens, 8, taps_count)],
        [shaped((tokens, channels), BF16)] + [shaped((8, channels))] * 3 + [shaped(heads_shape)],
        [wide(tokens), wide(8), wide(8), wide(8), full(heads_shape)],
        grid=(group + 1,),
        scratch=[pltpu.VMEM((state, tokens), F32)] + [pltpu.VMEM(heads_shape, F32)] * 2
        + [pltpu.VMEM((heads, state), F32)],
        name="outer", flops=3e9, nbytes=2e7,
    )
    returned = lax.ppermute(returned, "seq", [(s, s - 1) for s in range(1, seq)])

    there = [swap(part, 1, 0) for part in gathered]
    half_shape = (peers * part_rows, width)

    def decode(parts):
        return call(
            functools.partial(decode_kernel, peers), [me, *parts],
            [SMEM] + [full(coded_shape)] * peers, shaped(half_shape), full(half_shape),
            name="decode",
        )

    mine, other = decode(gathered), decode(there)
    weight_grad = jnp.where(
        me[0] % 2 == 0, jnp.concatenate([mine, other]), jnp.concatenate([other, mine])
    )

    def add_up(value, move, size):
        if size >= 4:
            one, two, three = move(value, 1), move(value, 2), move(value, 3)
            value, bit = (value + one) + (two + three), 4
        else:
            bit = 1
        while bit < size:
            value = value + move(value, bit)
            bit *= 2
        return value

    sums = add_up(sums, lambda v, k: swap(v, 0, k), dp)
    sums = add_up(sums, lambda v, k: swap(v, k, 0), seq)
    input_grad = lax.dynamic_update_slice_in_dim(
        input_grad, (tail + returned).astype(BF16), tokens - 8, axis=0
    )
    above = taps_count + 1
    head_at = inner + state
    return (
        input_grad[None],
        gate_grad[None],
        step_grad[None],
        weight_grad,
        sums[:above],
        sums[above, :inner],
        sums[above : above + 3, head_at : head_at + heads],
    )


def solution(mesh):
    return jax.shard_map(
        body,
        mesh=mesh,
        in_specs=(
            P("dp", "seq", None),
            P("dp", "seq", None),
            P("dp", None, "seq"),
            P(),
            P(),
            P(),
            P(),
            P(),
            P(),
            P("dp", None),
            P("dp", "seq", None),
        ),
        out_specs=(
            P("dp", "seq", None),
            P("dp", "seq", None),
            P("dp", None, "seq"),
            P("dp", None),
            P(),
            P(),
            P(),
        ),
        check_vma=False,
    )
```

```python
import functools

import jax
import jax.numpy as jnp
from jax import lax
from jax.experimental import pallas as pl
from jax.experimental.pallas import tpu as pltpu
from jax.sharding import PartitionSpec as P


F32 = jnp.float32
BF16 = jnp.bfloat16
HIGHEST = lax.Precision.HIGHEST
MASKED = -1e30
EPSILON = 1e-05
PAIR = 128
CODE = 120.0
TINY = 1e-30
VMEM = 28 * 1024 * 1024


NN = (((1,), (0,)), ((), ()))
NT = (((1,), (1,)), ((), ()))


def full(shape):
    zeros = (0,) * len(shape)
    return pl.BlockSpec(shape, lambda *_: zeros)


SMEM = pl.BlockSpec(memory_space=pltpu.SMEM)


def dot(a, b, dims):
    return lax.dot_general(a, b, dims, preferred_element_type=F32)


def split(x):
    high = x.astype(BF16)
    return high, (x - high.astype(F32)).astype(BF16)


def dot3(a, b, dims):
    (ah, al), (bh, bl) = a, b
    return dot(ah, bh, dims) + dot(ah, bl, dims) + dot(al, bh, dims)


def both(first, second, rows):
    width = first.shape[-1]
    return jnp.concatenate(
        [jnp.broadcast_to(first, (rows, width)), jnp.broadcast_to(second, (rows, width))], axis=0
    )


def choose(index, parts):
    out = parts[0]
    for k in range(1, len(parts)):
        out = jnp.where(index == k, parts[k], out)
    return out


def triangle(size, upper):
    row = lax.broadcasted_iota(jnp.int32, (size, size), 0)
    col = lax.broadcasted_iota(jnp.int32, (size, size), 1)
    return row <= col if upper else row >= col


def call(kernel, args, in_specs, out_shape, out_specs, grid=(1,), after=(), scratch=(),
         aliases=None):
    count, extra = len(args), len(after)

    def run(*refs):
        kernel(*refs[:count], *refs[count + extra :])

    return pl.pallas_call(
        run,
        grid=grid,
        in_specs=list(in_specs) + [pl.BlockSpec(memory_space=pl.ANY)] * extra,
        out_specs=out_specs,
        out_shape=out_shape,
        scratch_shapes=list(scratch),
        compiler_params=pltpu.CompilerParams(
            dimension_semantics=("arbitrary",) * len(grid), vmem_limit_bytes=VMEM
        ),
        input_output_aliases=aliases or {},
    )(*args, *after)


def shaped(shape, dtype=F32):
    return jax.ShapeDtypeStruct(shape, dtype)


def upright(flat):
    count = flat.shape[1]
    row = lax.broadcasted_iota(jnp.int32, (count, count), 0)
    col = lax.broadcasted_iota(jnp.int32, (count, count), 1)
    wide = jnp.broadcast_to(flat, (count, count))
    return jnp.sum(jnp.where(row == col, wide, 0.0), axis=1, keepdims=True)


def steps_kernel(
    step_ref, small_ref, filter_bias_ref, steps_ref, cums_ref, columns_ref, filter_row_ref, side_ref,
):
    bias, log = upright(small_ref[0:1, :]), upright(small_ref[1:2, :])
    raw = step_ref[...] + bias
    steps = jnp.maximum(raw, 0.0) + jnp.log1p(jnp.exp(-jnp.abs(raw)))
    rate = -jnp.exp(log)
    rates = rate * steps
    heads, size = raw.shape
    ones = jnp.where(triangle(size, True), 1.0, 0.0).astype(F32)
    cums = lax.dot_general(rates, ones, NN, precision=HIGHEST, preferred_element_type=F32)
    steps_ref[...] = steps
    cums_ref[...] = cums
    columns_ref[...] = jnp.concatenate([cums, jnp.zeros((PAIR - heads, size), F32)], axis=0).T
    filter_row_ref[...] = filter_bias_ref[...].reshape(filter_row_ref.shape)
    side_ref[0] = jnp.broadcast_to(bias, side_ref.shape[1:])
    side_ref[1] = jnp.broadcast_to(rate, side_ref.shape[1:])
    side_ref[2] = jnp.broadcast_to(upright(small_ref[2:3, :]), side_ref.shape[1:])


def extend(halo, raw):
    return jnp.concatenate([halo.astype(F32), raw.astype(F32)], axis=0)


def activation(extended, taps, bias):
    width = taps.shape[0]
    start = 8 - width + 1
    size = extended.shape[0] - 8
    filtered = bias + taps[0:1] * extended[start : start + size]
    for k in range(1, width):
        filtered = filtered + taps[k : k + 1] * extended[start + k : start + k + size]
    gate = jax.nn.sigmoid(filtered)
    active = filtered * gate
    return active, gate + active * (1.0 - gate)


def filter_kernel(
    halo_ref, raw_ref, taps_ref, bias_ref,
    side_halo_ref, side_raw_ref, side_taps_ref, side_bias_ref, steps_ref, cums_ref,
    slope_ref, features_ref, side_slope_ref, side_features_ref, sides_ref, *rest,
):
    chunks, (key_high, key_low) = rest[:-2], rest[-2:]
    i = pl.program_id(0)
    size, lanes = raw_ref.shape
    units = lanes // PAIR
    extra = 16

    @pl.when(i == 0)
    def _():
        for u in range(side_raw_ref.shape[1] // PAIR):
            at = slice(u * PAIR, (u + 1) * PAIR)
            active, slope = activation(
                extend(side_halo_ref[:, at], side_raw_ref[:, at]), side_taps_ref[:, at],
                side_bias_ref[:, at],
            )
            side_slope_ref[:, at] = slope
            side_features_ref[at, :] = active.T
            sides_ref[:, at] = active
            if u == 0:
                key_high[...], key_low[...] = split(active)

    slot = i ^ (lax.axis_index("seq") % len(chunks))
    keys = (key_high[...], key_low[...])
    lasts = []
    states = []
    for u in range(units):
        at = slice(u * PAIR, (u + 1) * PAIR)
        active, slope = activation(
            extend(halo_ref[:, at], raw_ref[:, at]), taps_ref[:, at], bias_ref[:, at]
        )
        slope_ref[:, at] = slope
        features = active.T
        features_ref[at, :] = features
        rows = []
        for j in range(2):
            head = (i * units + u) * 2 + j
            cums = cums_ref[pl.ds(head, 1), :]
            last = cums[:, size - 1 :]
            lasts.append(jnp.broadcast_to(jnp.exp(last), (1, PAIR)))
            rows.append(steps_ref[pl.ds(head, 1), :] * jnp.exp(last - cums))
        scaled = features * both(rows[0], rows[1], PAIR // 2)
        states.append(dot3(split(scaled), keys, NN).astype(BF16))
    lasts.append(jnp.zeros((extra - len(lasts), PAIR), F32))
    decay_high, decay_low = split(jnp.concatenate(lasts, axis=0))
    for k, chunk in enumerate(chunks):

        @pl.when(slot == k)
        def _():
            for u in range(units):
                chunk[u * PAIR : (u + 1) * PAIR, :] = states[u]
            chunk[lanes : lanes + extra, :] = decay_high
            chunk[lanes + extra :, :] = decay_low


def scan_chunk(group, reverse, width, decays, parts, carry_ref, scratch, total_ref):
    here = lax.axis_index("seq") % group
    rows_all = total_ref.shape[0] if total_ref is not None else carry_ref.shape[0]
    order = range(group - 1, -1, -1) if reverse else range(group)
    fall = [
        choose(here ^ p, [d[:16, :].astype(F32) + d[16:, :].astype(F32) for d in decays])
        for p in range(group)
    ]
    for h in range(rows_all // width):
        rows = pl.ds(h * width, width)
        if carry_ref is None:
            running = jnp.zeros((width, parts[0].shape[1]), F32)
        else:
            running = carry_ref[rows, :].astype(F32)
        for n, p in enumerate(order):
            if scratch is not None:
                scratch[p, rows, :] = running
                if n == group - 1:
                    break
            term = choose(here ^ p, [part[rows, :] for part in parts]).astype(F32)
            running = term + fall[p][h : h + 1, :] * running
        if total_ref is not None:
            total_ref[rows, :] = running.astype(BF16)


def carry_kernel(group, reverse, width, *refs):
    decays, parts, out_ref = refs[:group], refs[group : 2 * group], refs[2 * group]
    scan_chunk(group, reverse, width, decays, parts, None, None, out_ref)


def spread_kernel(group, reverse, width, *refs):
    decays, parts, carry_ref = refs[:group], refs[group : 2 * group], refs[2 * group]
    outs, scratch = refs[2 * group + 1 : 3 * group + 1], refs[3 * group + 1]
    scan_chunk(group, reverse, width, decays, parts, carry_ref, scratch, None)
    here = lax.axis_index("seq") % group
    for k in range(group):
        outs[k][...] = scratch[here ^ k].astype(BF16)


class Exchange:
    def __init__(self, seq, group, rows, state, head_dim, reverse):
        self.seq, self.group, self.reverse = seq, group, reverse
        self.rows, self.state, self.head_dim = rows, state, head_dim

    def swap(self, value, k):
        return lax.ppermute(value, "seq", [(s, s ^ k) for s in range(self.seq)])

    def send(self, chunks):
        self.got = [chunks[0]] + [self.swap(chunks[k], k) for k in range(1, self.group)]

    def specs(self):
        row = self.rows // 32
        return (
            [pl.BlockSpec((32, self.state), lambda i: (row, 0))] * self.group
            + [pl.BlockSpec((self.rows, self.state), lambda i: (0, 0))] * self.group
        )

    def total(self, decays, after=()):
        self.decays = decays
        groups = self.seq // self.group
        shape = (self.rows, self.state)
        total = call(
            functools.partial(carry_kernel, self.group, self.reverse, self.head_dim),
            [*decays, *self.got], self.specs(), shaped(shape, BF16), full(shape),
            after=after,
        )
        g = self.group
        ways = (
            [(s, s - g) for s in range(g, self.seq)]
            if self.reverse
            else [(s, s + g) for s in range(self.seq - g)]
        )
        carry = lax.ppermute(total, "seq", ways)
        if groups > 2:
            product = 1.0
            for d in decays:
                tail = d[self.rows :].astype(F32)
                product = product * (tail[:16] + tail[16:])
            product = jnp.repeat(product[: self.rows // self.head_dim], self.head_dim, axis=0)
            for _ in range(groups - 2):
                step = total.astype(F32) + product * carry.astype(F32)
                carry = lax.ppermute(step.astype(BF16), "seq", ways)
        self.carry = carry
        return total

    def spread(self, after=()):
        shape = (self.rows, self.state)
        g = self.group
        self.outs = call(
            functools.partial(spread_kernel, g, self.reverse, self.head_dim),
            [*self.decays, *self.got, self.carry],
            self.specs() + [full(shape)],
            [shaped(shape, BF16)] * g, [full(shape)] * g, after=after,
            scratch=[pltpu.VMEM((g,) + shape, F32)],
        )
        return [self.outs[0]] + [self.swap(self.outs[k], k) for k in range(1, g)]


def column_of(columns_ref, first):
    return pltpu.roll(columns_ref[...], PAIR - first, 1)


def falls(row, column, half, low):
    first = jnp.exp(jnp.where(low[0], row - column[:half], MASKED))
    second = jnp.exp(jnp.where(low[1], row[:, half:] - column[half:], MASKED))
    return first, second


def masks(size):
    half = size // 2
    row = lax.broadcasted_iota(jnp.int32, (half, size), 0)
    col = lax.broadcasted_iota(jnp.int32, (half, size), 1)
    return row <= col, triangle(half, True)


def scores(sides_ref, score_ref):
    sides = sides_ref[...]
    state = sides.shape[1] // 2
    score_ref[...] = dot3(split(sides[:, :state]), split(sides[:, state:]), NT)


def pad_left(value, size):
    return jnp.concatenate([jnp.zeros((value.shape[0], size), F32), value], axis=1)


def inside_kernel(
    first_head, skip_ref, features_ref, sides_ref, steps_ref, cums_ref, columns_ref, *refs
):
    out_ref, score_ref = refs[-2:]
    i = pl.program_id(0)

    @pl.when(i == 0)
    def _():
        scores(sides_ref, score_ref)

    size = score_ref.shape[0]
    low = masks(size)
    span = PAIR // 2
    half = size // 2
    units = out_ref.shape[0] // span
    base = first_head + i * units
    columns = column_of(columns_ref, base)
    for j in range(units):
        part = slice(j * span, (j + 1) * span)
        values = features_ref[part, :]
        scaled = values * steps_ref[pl.ds(base + j, 1), :]
        fall = falls(cums_ref[pl.ds(base + j, 1), :], columns[:, j : j + 1], half, low)
        ah, al = split(score_ref[:half, :] * fall[0])
        bh, bl = split(score_ref[half:, half:] * fall[1])
        xh, xl = split(scaled)
        stack = jnp.concatenate([xh, xl], axis=0)
        first = dot(stack[:, :half], ah, NN)
        second = dot(stack[:, half:], bh, NN)
        inside = first[:span] + first[span:] + dot(xh[:, :half], al, NN)
        later = second[:span] + second[span:] + dot(xh[:, half:], bl, NN)
        inside = inside + pad_left(later, half)
        out_ref[part, :] = inside + skip_ref[base + j] * values


def inner_kernel(
    first_head, features_ref, sides_ref, steps_ref, cums_ref, columns_ref,
    cotangent_ref, entering_ref, *refs
):
    before, refs = refs[:-6], refs[-6:]
    grad_ref, direct_ref, total_out, carried_out, score_ref, total_ref = refs
    i = pl.program_id(0)

    @pl.when(i == 0)
    def _():
        scores(sides_ref, score_ref)
        if before:
            direct_ref[...] = before[1][...]
            total_ref[...] = before[2][...]
            carried_out[...] = before[3][...]
        else:
            direct_ref[...] = jnp.zeros_like(direct_ref)
            total_ref[...] = jnp.zeros_like(total_ref)
            carried_out[...] = jnp.zeros_like(carried_out)

    size = score_ref.shape[0]
    low = masks(size)
    span = PAIR // 2
    half = size // 2
    units = grad_ref.shape[0] // span
    base = first_head + i * units
    columns = column_of(columns_ref, base)
    decayed = []
    for j in range(units):
        part = slice(j * span, (j + 1) * span)
        values = features_ref[part, :]
        cotangent = cotangent_ref[part, :]
        scaled = values * steps_ref[pl.ds(base + j, 1), :]
        row = cums_ref[pl.ds(base + j, 1), :]
        fall = falls(row, columns[:, j : j + 1], half, low)
        ah, al = split(score_ref[:half, :] * fall[0])
        bh, bl = split(score_ref[half:, half:] * fall[1])
        gh, gl = split(cotangent)
        xh, xl = split(scaled.T)
        stack = jnp.concatenate([gh, gl], axis=0)
        first = dot(stack, ah, NT)
        second = dot(stack[:, half:], bh, NT)
        grad_ref[part, :half] = first[:span] + first[span:] + dot(gh, al, NT)
        grad_ref[part, half:] = second[:span] + second[span:] + dot(gh[:, half:], bl, NT)
        left = jnp.concatenate([xh, xh, xl], axis=1)
        right = jnp.concatenate([gh, gl, gh], axis=0)
        total_ref[:half, :] += dot(left[:half], right, NN) * fall[0]
        total_ref[half:, half:] += dot(left[half:], right[:, half:], NN) * fall[1]
        direct_ref[pl.ds(base + j, 1), :] = jnp.sum(cotangent * values, axis=0, keepdims=True)
        decayed.append(cotangent * jnp.exp(row))
    ch, cl = split(jnp.concatenate(decayed, axis=0))
    entering = entering_ref[...].astype(F32).T.astype(BF16)
    carried_out[...] += dot(entering, ch, NN) + dot(entering, cl, NN)

    @pl.when(i == pl.num_programs(0) - 1)
    def _():
        total_out[...] = total_ref[...]


def norm_kernel(group, dp, halves, *refs):
    states, refs = refs[:group], refs[group:]
    grads, refs = refs[:dp], refs[dp:]
    (local_ref, gate_ref, cums_ref, query_ref, weight_ref), refs = refs[:5], refs[5:]
    (gated_ref, open_ref, slope_ref, grad_ref, row_ref, entering_ref), refs = refs[:6], refs[6:]
    lows, refs = refs[: halves * dp], refs[halves * dp :]
    gated_s, square_s, cross_s = refs
    phase, b = pl.program_id(0), pl.program_id(1)
    lanes = gate_ref.shape[1]
    units = lanes // PAIR
    half = PAIR // 2
    blocks = pl.num_programs(1)
    at_seq, at_dp = lax.axis_index("seq"), lax.axis_index("dp")

    @pl.when(phase == 0)
    def _():
        queries = split(query_ref[...])
        slot = (at_seq % group) ^ b
        source = at_dp ^ b
        scale = choose(source, [g[lanes : lanes + 1, :] for g in grads]).astype(F32) * (1.0 / CODE)
        square = cross = 0.0
        for u in range(units):
            at = slice(u * PAIR, (u + 1) * PAIR)
            here = pl.ds(b * lanes + u * PAIR, PAIR)
            head = (b * units + u) * 2
            exps = both(
                jnp.exp(cums_ref[pl.ds(head, 1), :]), jnp.exp(cums_ref[pl.ds(head + 1, 1), :]), half
            )
            entering = choose(slot, [s[at, :] for s in states])
            entering_ref[at, :] = entering
            carried = dot(entering, queries[0], NN) + dot(entering, queries[1], NN)
            scanned = local_ref[at, :] + carried * exps
            z = gate_ref[:, at].astype(F32).T
            opened = jax.nn.sigmoid(z)
            through = z * opened
            gated = scanned * through
            grad = jnp.log2(choose(source, [g[at, :] for g in grads]).astype(F32)) * scale
            gated_s[here, :] = gated
            gated_ref[at, :] = gated
            open_ref[at, :] = through
            slope_ref[at, :] = scanned * (opened + through * (1.0 - opened))
            grad_ref[at, :] = grad
            square = square + jnp.sum(gated * gated, axis=0, keepdims=True)
            cross = cross + jnp.sum(gated * (grad * weight_ref[at, :]), axis=0, keepdims=True)

        @pl.when(b == 0)
        def _():
            square_s[...] = square
            cross_s[...] = cross

        @pl.when(b > 0)
        def _():
            square_s[...] += square
            cross_s[...] += cross

    @pl.when(phase == 1)
    def _():
        share = 1.0 / (blocks * lanes)
        inverse = lax.rsqrt(square_s[...] * share + EPSILON)
        row_ref[0:1, :] = inverse
        row_ref[1:2, :] = inverse * inverse * inverse * (cross_s[...] * share)
        results = []
        for u in range(units):
            here = pl.ds(b * lanes + u * PAIR, PAIR)
            weight = weight_ref[u * PAIR : (u + 1) * PAIR, :]
            results.append((gated_s[here, :] * inverse * weight).astype(BF16))
        low = jnp.concatenate(results, axis=0)
        part = lanes // halves
        for ks in range(halves):
            for kd in range(dp):
                for n in range(halves):

                    @pl.when(((at_dp ^ b) == kd) & ((n ^ (at_seq % halves)) == ks))
                    def _():
                        lows[ks * dp + kd][...] = low[n * part : (n + 1) * part]


def turn_kernel(
    group, gated_ref, open_ref, slope_ref, grad_ref, row_ref, cums_ref, sides_ref, weight_ref,
    cotangent_ref, gate_grad_ref, norm_ref, sum_ref, *entries,
):
    b = pl.program_id(0)
    lanes, size = gated_ref.shape
    units = lanes // PAIR
    half = PAIR // 2
    inverse, shift = row_ref[0:1, :], row_ref[1:2, :]
    sides = split(sides_ref[...])
    ones = jnp.ones((8, size), BF16)
    heads = []
    for u in range(units):
        at = slice(u * PAIR, (u + 1) * PAIR)
        head = (b * units + u) * 2
        exps = both(
            jnp.exp(cums_ref[pl.ds(head, 1), :]), jnp.exp(cums_ref[pl.ds(head + 1, 1), :]), half
        )
        gated = gated_ref[at, :]
        scaled = inverse * grad_ref[at, :]
        product = split(gated * scaled)
        norm_ref[:, at] = dot(ones, product[0], NT) + dot(ones, product[1], NT)
        gated_grad = scaled * weight_ref[at, :] - gated * shift
        sums = gated_grad * gated
        for j in range(2):
            sum_ref[pl.ds(head + j, 1), :] = jnp.sum(
                sums[j * half : (j + 1) * half], axis=0, keepdims=True
            )
        cotangent = gated_grad * open_ref[at, :]
        cotangent_ref[at, :] = cotangent
        gate_grad_ref[:, at] = (gated_grad * slope_ref[at, :]).T.astype(BF16)
        heads.append(dot3(split(cotangent * exps), sides, NN).astype(BF16))
    entry = (lax.axis_index("seq") % group) ^ b
    for k in range(group):

        @pl.when(entry == k)
        def _():
            for u in range(units):
                entries[k][u * PAIR : (u + 1) * PAIR, :] = heads[u]


def outer_kernel(group, skip_ref, *refs):
    states, refs = refs[:group], refs[group:]
    (
        features_ref, side_features_ref, steps_ref, cums_ref, cotangent_ref, grad_ref,
        total_ref, carried_ref, entering_ref, row_refs, direct_ref, step_in_ref,
        head_side_ref, norm_ref, slope_ref, raw_ref, halo_ref, taps_ref,
        side_slope_ref, side_raw_ref, side_halo_ref, side_taps_ref,
        out_ref, tail_ref, back_ref, sums_ref, step_ref,
        key_grad_s, value_s, end_s, decay_s,
    ) = refs
    i = pl.program_id(0)
    blocks = pl.num_programs(0) - 1
    half = PAIR // 2
    size, lanes = raw_ref.shape
    units = lanes // PAIR
    heads = steps_ref.shape[0]
    state = side_features_ref.shape[0] // 2

    @pl.when(i == 0)
    def _():
        key_grad_s[...] = jnp.zeros_like(key_grad_s)

    def filtered(grad, slope, halo, raw, taps, at):
        df = grad.T * slope
        width = taps.shape[0]
        longer = jnp.concatenate([df, jnp.zeros((8, PAIR), F32)], axis=0)
        ahead = jnp.concatenate([jnp.zeros((8, PAIR), F32), df[0:8]], axis=0)
        extended = extend(halo, raw)
        start = 8 - width + 1
        last = width - 1
        own = taps[0:1] * longer[last : last + size]
        back = taps[0:1] * ahead[last : last + 8]
        sums = [jnp.sum(df * extended[start : start + size], axis=0, keepdims=True)]
        for k in range(1, width):
            own = own + taps[k : k + 1] * longer[last - k : last - k + size]
            back = back + taps[k : k + 1] * ahead[last - k : last - k + 8]
            sums.append(
                jnp.sum(df * extended[start + k : start + k + size], axis=0, keepdims=True)
            )
        sums.append(jnp.sum(df, axis=0, keepdims=True))
        out_ref[:, at] = own.astype(BF16)
        tail_ref[:, at] = own[size - 8 :]
        back_ref[:, at] = back
        return sums

    @pl.when(i < blocks)
    def _():
        b = jnp.minimum(i, blocks - 1)
        slot = (lax.axis_index("seq") % group) ^ b
        keys = split(side_features_ref[:state, :])
        total = 0.0
        for u in range(units):
            at = slice(u * PAIR, (u + 1) * PAIR)
            ending = choose(slot, [s[at, :] for s in states])
            from_end = dot(ending, keys[0], NN) + dot(ending, keys[1], NN)
            tops, steps = [], []
            first = (b * units + u) * 2
            for j in range(2):
                cums = cums_ref[pl.ds(first + j, 1), :]
                tops.append(jnp.exp(cums[:, size - 1 :] - cums))
                steps.append(steps_ref[pl.ds(first + j, 1), :])
            top = both(tops[0], tops[1], half)
            step = both(steps[0], steps[1], half)
            values = features_ref[at, :]
            from_end = from_end * top
            grad = grad_ref[at, :] + from_end
            scaled = values * step
            sh, sl = split(scaled * top)
            ends = ending.astype(F32)
            turned = ends.T.astype(BF16)
            total = total + dot(turned, sh, NN) + dot(turned, sl, NN)
            by_value = values * grad
            by_end = scaled * from_end
            product = ends * entering_ref[at, :].astype(F32)
            skips = []
            for j in range(2):
                part = slice(j * half, (j + 1) * half)
                row = pl.ds(first + j, 1)
                value_s[row, :] = jnp.sum(by_value[part], axis=0, keepdims=True)
                end_s[row, :] = jnp.sum(by_end[part], axis=0, keepdims=True)
                decay_s[row, :] = jnp.sum(product[part], axis=0, keepdims=True)
                skips.append(
                    skip_ref[first + j]
                    * cotangent_ref[u * PAIR + j * half : u * PAIR + (j + 1) * half, :]
                )
            where = pl.ds(pl.multiple_of(b * lanes + u * PAIR, PAIR), PAIR)
            sums = filtered(
                jnp.concatenate(skips, axis=0) + grad * step, slope_ref[:, at], halo_ref[:, at],
                raw_ref[:, at], taps_ref[:, at], where,
            )
            sums.append(norm_ref[0:1, at])
            sums_ref[:, where] = jnp.concatenate(
                sums + [jnp.zeros((8 - len(sums), PAIR), F32)], axis=0
            )
        key_grad_s[...] += total

    @pl.when(i == blocks)
    def _():
        score = split(total_ref[...])
        inner = blocks * lanes
        steps, cums = steps_ref[...], cums_ref[...]
        values = value_s[...]
        direct = direct_ref[...]
        base = row_refs[...] - head_side_ref[2][:, 0:1] * direct - steps * values
        ones = jnp.where(triangle(size, False), 1.0, 0.0).astype(F32)
        rate_grad = lax.dot_general(base, ones, NN, precision=HIGHEST, preferred_element_type=F32)
        ended = jnp.sum(end_s[...], axis=1, keepdims=True)
        kept = jnp.exp(cums[:, size - 1 :]) * jnp.sum(decay_s[...], axis=1, keepdims=True)
        rate_grad = rate_grad + (ended + kept)
        bias, rate = head_side_ref[0][:, 0:1], head_side_ref[1][:, 0:1]
        step_grad = (values + rate_grad * rate) * jax.nn.sigmoid(step_in_ref[...] + bias)
        step_ref[...] = step_grad
        row = lax.broadcasted_iota(jnp.int32, (heads, PAIR), 0)
        col = lax.broadcasted_iota(jnp.int32, (heads, PAIR), 1)
        head_rows = []
        for source in (step_grad, rate_grad * steps * rate, direct):
            column = jnp.sum(source, axis=1, keepdims=True)
            head_rows.append(jnp.sum(jnp.where(row == col, column, 0.0), axis=0, keepdims=True))
        keys = side_features_ref[:state, :]
        queries = side_features_ref[state:, :]
        key_grad = dot3(split(queries), score, NT) + key_grad_s[...]
        query_grad = dot3(split(keys), score, NN) + carried_ref[...]
        for u, grad in enumerate((key_grad, query_grad)):
            at = slice(u * PAIR, (u + 1) * PAIR)
            where = slice(inner + u * PAIR, inner + (u + 1) * PAIR)
            sums = filtered(
                grad, side_slope_ref[:, at], side_halo_ref[:, at], side_raw_ref[:, at],
                side_taps_ref[:, at], where,
            )
            sums_ref[:, where] = jnp.concatenate(sums + head_rows, axis=0)


def encode(values):
    scale = jnp.max(jnp.abs(values), axis=0, keepdims=True) * 1.01 + TINY
    scale = scale.astype(BF16)
    coded = jnp.exp2(values * (CODE / scale.astype(F32))).astype(BF16)
    return coded, jnp.broadcast_to(scale, (16, values.shape[1]))


def project_kernel(count, weight_ref, *refs):
    cotangents, outs = refs[:count], refs[count:]
    rows = weight_ref.shape[0]
    for k in range(count):
        coded, scale = encode(dot(weight_ref[...], cotangents[k][...], NT))
        outs[k][:rows, :] = coded
        outs[k][rows:, :] = scale


def outer_product_kernel(count, peers, *refs):
    lows, cotangents, keep_ref, send_ref = refs[:count], refs[count : 2 * count], *refs[-2:]
    width = keep_ref.shape[1]
    tile = 2 * PAIR
    tiles = []
    for n in range(0, width, tile):
        part = dot(lows[0][...], cotangents[0][:, n : n + tile], NN)
        for k in range(1, count):
            part = part + dot(lows[k][...], cotangents[k][:, n : n + tile], NN)
        tiles.append(part)
    total = jnp.concatenate(tiles, axis=1)
    rows = 2 * keep_ref.shape[0] // peers
    here = lax.axis_index("seq") // 2
    for p in range(peers):
        piece = total[p * rows : (p + 1) * rows]
        for j in range(peers // 2):
            at = slice(j * rows, (j + 1) * rows)

            @pl.when((here ^ p) == 2 * j)
            def _():
                keep_ref[at, :] = piece

            @pl.when((here ^ p) == 2 * j + 1)
            def _():
                send_ref[at, :] = piece.astype(BF16)


def merge_kernel(keep_ref, part_ref, own_ref, *sends):
    rows = own_ref.shape[0]
    own_ref[...] = keep_ref[:rows, :] + part_ref[:rows, :].astype(F32)
    for j, send in enumerate(sends):
        at = slice((j + 1) * rows, (j + 2) * rows)
        send[...] = (keep_ref[at, :] + part_ref[at, :].astype(F32)).astype(BF16)


def fold_kernel(keep_ref, *refs):
    parts, out_ref = refs[:-1], refs[-1]
    values = keep_ref[...]
    for part in parts:
        values = values + part[...].astype(F32)
    width = keep_ref.shape[1]
    scale = (jnp.max(jnp.abs(values), axis=1, keepdims=True) * 1.01 + TINY).astype(BF16)
    scale = scale.astype(F32)
    out_ref[:, :width] = jnp.exp2(values * (CODE / scale)).astype(BF16)
    out_ref[:, width:] = jnp.broadcast_to(scale, (values.shape[0], PAIR)).astype(BF16)


def decode_kernel(peers, other, joined, *refs):
    parts, out_ref, scratch, sem = refs[: 2 if joined else peers], refs[-3], refs[-2], refs[-1]
    half = out_ref.shape[0] // 2
    width = out_ref.shape[1]
    rows = half // peers
    at_seq = lax.axis_index("seq")
    here = at_seq // 2
    start = ((at_seq % 2) ^ other) * half
    together = 1
    while rows * together % 8:
        together *= 2
    copies = []
    for p in range(peers):
        slot = here ^ p
        if joined:
            place = jnp.maximum(slot - 1, 0)
            coded = choose(jnp.minimum(slot, 1), [parts[0][...], parts[1][place]])
        else:
            coded = choose(slot, [part[...] for part in parts])
        scale = coded[:, width : width + 1].astype(F32) * (1.0 / CODE)
        scratch[p * rows : (p + 1) * rows, :] = jnp.log2(coded[:, :width].astype(F32)) * scale
        if (p + 1) % together == 0:
            size = rows * together
            first = (p + 1) * rows - size
            copies.append(
                pltpu.make_async_copy(
                    scratch.at[pl.ds(first, size), :],
                    out_ref.at[pl.ds(pl.multiple_of(start + first, 8), size), :],
                    sem.at[len(copies)],
                )
            )
            copies[-1].start()
    for copy in copies:
        copy.wait()


def body(
    conv_input, gate_input, step_input, filter_taps, filter_bias, step_bias, decay_log,
    skip_gain, norm_weight, output_weight, output_grad,
):
    seq, dp = lax.axis_size("seq"), lax.axis_size("dp")
    group = dp
    raw, gate, step_rows, cotangent = conv_input[0], gate_input[0], step_input[0], output_grad[0]
    tokens, channels = raw.shape
    inner = gate.shape[1]
    heads = step_rows.shape[0]
    head_dim = inner // heads
    state = (channels - inner) // 2
    width = cotangent.shape[1]
    taps_count = filter_taps.shape[0]
    rows = inner // group
    side = 2 * state
    both_axes = ("seq", "dp")

    def swap(value, seq_bits, dp_bits):
        pairs = [
            (s * dp + d, (s ^ seq_bits) * dp + (d ^ dp_bits)) for s in range(seq) for d in range(dp)
        ]
        return lax.ppermute(value, both_axes, pairs)

    tail = raw[-8:]
    halo = lax.ppermute(tail, "seq", [(s, s + 1) for s in range(seq - 1)])

    far = dp // 2
    known = {(0, 0): cotangent}
    known[(0, far)] = swap(cotangent, 0, far)
    known[(1, 0)] = swap(cotangent, 1, 0)

    column = lambda v: v.reshape(-1, 1)
    heads_shape, sides_shape = (heads, tokens), (3, heads, PAIR)
    steps, cums, columns, bias_row, head_sides = call(
        steps_kernel, [step_rows, jnp.stack([step_bias, decay_log, skip_gain]), filter_bias],
        [full(heads_shape), full((3, heads)), full((channels,))],
        [shaped(heads_shape), shaped(heads_shape), shaped((tokens, PAIR)), shaped((1, channels)),
         shaped(sides_shape)],
        [full(heads_shape), full(heads_shape), full((tokens, PAIR)), full((1, channels)),
         full(sides_shape)],
    )

    at_chunk = lambda i: (0, i)
    at_side = lambda i: (0, inner // side)
    payload = (rows + 32, state)
    slope, features, side_slope, side_features, sides, *chunks = call(
        filter_kernel,
        [halo, raw, filter_taps, bias_row, halo, raw, filter_taps, bias_row, steps, cums],
        [pl.BlockSpec((n, rows), at_chunk) for n in (8, tokens, taps_count, 1)]
        + [pl.BlockSpec((n, side), at_side) for n in (8, tokens, taps_count, 1)]
        + [full(heads_shape)] * 2,
        [
            shaped((tokens, inner)), shaped((inner, tokens)), shaped((tokens, side)),
            shaped((side, tokens)), shaped((tokens, side)),
        ]
        + [shaped(payload, BF16)] * group,
        [
            pl.BlockSpec((tokens, rows), at_chunk), pl.BlockSpec((rows, tokens), lambda i: (i, 0)),
            full((tokens, side)), full((side, tokens)), full((tokens, side)),
        ]
        + [full(payload)] * group,
        grid=(group,), scratch=[pltpu.VMEM((tokens, state), BF16)] * 2,
    )

    forward = Exchange(seq, group, rows, state, head_dim, False)
    forward.send(chunks)
    decays = forward.got
    known[(0, 1)] = swap(known[(0, 0)], 0, 1)

    units = 2 * PAIR
    parts = inner // units // 2
    pair_shape = (units, tokens)

    any_space = pl.BlockSpec(memory_space=pl.ANY)

    def inside(n, before, after):
        return call(
            functools.partial(inside_kernel, n * heads // 2),
            [skip_gain, features, sides, steps, cums, columns, *before],
            [
                SMEM, pl.BlockSpec(pair_shape, lambda i: (n * parts + i, 0)), full((tokens, side)),
                full(heads_shape), full(heads_shape), full((tokens, PAIR)),
            ] + [any_space] * len(before),
            shaped((inner, tokens)), pl.BlockSpec(pair_shape, lambda i: (n * parts + i, 0)),
            grid=(parts,), after=after, scratch=[pltpu.VMEM((tokens, tokens), F32)],
            aliases={6: 0} if before else None,
        )

    known[(0, far)], _ = lax.optimization_barrier((known[(0, far)], side_slope))
    known[(0, far + 1)] = swap(known[(0, far)], 0, 1)

    piece = (rows + 16, tokens)
    served = call(
        functools.partial(project_kernel, dp),
        [output_weight] + [known[(0, k)] for k in range(dp)],
        [full((rows, width))] + [full((tokens, width))] * dp,
        [shaped(piece, BF16)] * dp, [full(piece)] * dp, after=(side_slope,),
    )
    grads = [served[0]] + [swap(served[k], 0, k) for k in range(1, dp)]
    total = forward.total(decays, (served[0],))
    local = inside(0, (), (total,))
    entering = forward.spread((local,))
    local = inside(1, (local,), (forward.outs[0],))

    halves = 2
    known[(1, 0)], known[(0, 1)], _ = lax.optimization_barrier(
        (known[(1, 0)], known[(0, 1)], forward.outs[0])
    )
    known[(1, far)] = swap(known[(1, 0)], 0, far)
    known[(1, 1)] = swap(known[(1, 0)], 0, 1)
    entry_shape, low_shape = (rows, state), (rows // halves, tokens)
    gain = column(norm_weight)
    norm_in = lambda p, b: jnp.where(p == 0, b, group - 1)
    norm_rows = pl.BlockSpec((rows, tokens), lambda p, b: (norm_in(p, b), 0))
    row_shape = (8, tokens)
    gated, opened, gate_slope, grad, norm_row, entered, *lows = call(
        functools.partial(norm_kernel, group, dp, halves),
        [*entering, *grads, local, gate, cums, side_features, gain],
        [full(entry_shape)] * group + [full(piece)] * dp
        + [
            norm_rows,
            pl.BlockSpec((tokens, rows), lambda p, b: (0, norm_in(p, b))),
            full(heads_shape),
            pl.BlockSpec((state, tokens), lambda p, b: (1, 0)),
            pl.BlockSpec((rows, 1), lambda p, b: (b, 0)),
        ],
        [shaped((inner, tokens))] * 4
        + [shaped(row_shape), shaped((inner, state), BF16)]
        + [shaped(low_shape, BF16)] * (halves * dp),
        [norm_rows] * 4
        + [full(row_shape), pl.BlockSpec((rows, state), lambda p, b: (norm_in(p, b), 0))]
        + [full(low_shape)] * (halves * dp),
        grid=(2, group),
        scratch=[pltpu.VMEM((inner, tokens), F32)] + [pltpu.VMEM((1, tokens), F32)] * 2,
    )
    chunk_spec = pl.BlockSpec((rows, tokens), lambda i: (i, 0))
    scan_grad, gate_grad, norm_grad, gated_sums, *entries = call(
        functools.partial(turn_kernel, group),
        [gated, opened, gate_slope, grad, norm_row, cums, sides, gain],
        [chunk_spec] * 4
        + [
            full(row_shape), full(heads_shape), pl.BlockSpec((tokens, state), lambda i: (0, 1)),
            pl.BlockSpec((rows, 1), lambda i: (i, 0)),
        ],
        [
            shaped((inner, tokens)), shaped((tokens, inner), BF16), shaped((8, inner)),
            shaped(heads_shape),
        ]
        + [shaped(entry_shape, BF16)] * group,
        [
            chunk_spec, pl.BlockSpec((tokens, rows), at_chunk), pl.BlockSpec((8, rows), at_chunk),
            full(heads_shape),
        ]
        + [full(entry_shape)] * group,
        grid=(group,),
    )

    known[(1, far)], _ = lax.optimization_barrier((known[(1, far)], scan_grad))
    known[(1, far + 1)] = swap(known[(1, far)], 0, 1)
    sent = [lows[0]] + [None] * (halves * dp - 1)
    for n in low_order(dp):
        sent[n] = swap(lows[n], n // dp, n % dp)
    backward = Exchange(seq, group, rows, state, head_dim, True)
    backward.send(entries)

    def inner_call(n, before, after):
        pair_spec = pl.BlockSpec(pair_shape, lambda i: (n * parts + i, 0))
        kept = [full(heads_shape), full((tokens, tokens)), full((state, tokens))]
        return call(
            functools.partial(inner_kernel, n * heads // 2),
            [features, sides, steps, cums, columns, scan_grad, entered, *before],
            [
                pair_spec, full((tokens, side)), full(heads_shape), full(heads_shape),
                full((tokens, PAIR)), pair_spec,
                pl.BlockSpec((units, state), lambda i: (n * parts + i, 0)),
            ] + ([any_space] + kept if before else []),
            [
                shaped((inner, tokens)), shaped(heads_shape), shaped((tokens, tokens)),
                shaped((state, tokens)),
            ],
            [pair_spec] + kept,
            grid=(parts,), after=after, scratch=[pltpu.VMEM((tokens, tokens), F32)] * 2,
            aliases={7: 0} if before else None,
        )

    first_half = inner_call(0, (), ())

    peers = seq // halves
    count = halves * dp
    part_rows = rows // halves // peers
    both_rows = (peers // 2 * part_rows, width)
    keep, send = call(
        functools.partial(outer_product_kernel, count, peers),
        [*sent] + [known[(n // dp, n % dp)] for n in range(count)],
        [full(low_shape)] * count + [full((tokens, width))] * count,
        [shaped(both_rows), shaped(both_rows, BF16)], [full(both_rows)] * 2, after=(first_half[1],),
    )
    near = swap(send, halves, 0)
    total = backward.total(decays, (keep,))
    scaled_grad, direct_sums, score_grad, carried = inner_call(1, first_half, (total,))
    part_shape = (part_rows, width)
    keep, *sends = call(
        merge_kernel, [keep, near], [full(both_rows)] * 2,
        [shaped(part_shape)] + [shaped(part_shape, BF16)] * (peers // 2 - 1),
        [full(part_shape)] * (peers // 2), after=(direct_sums,),
    )
    arrived = [swap(send, 2 * halves * (j + 1), 0) for j, send in enumerate(sends)]
    ending = backward.spread((keep,))

    coded_shape = (part_rows, width + PAIR)
    coded = call(
        fold_kernel, [keep, *arrived], [full(part_shape)] * (peers // 2),
        shaped(coded_shape, BF16), full(coded_shape), after=(backward.outs[0],),
    )
    passed = {k: swap(coded, halves * k, 0) for k in range(peers - 1, 0, -1)}
    gathered = [coded] + [passed[k] for k in range(1, peers)]

    last = lambda i: jnp.minimum(i, group - 1)
    chunk_rows = lambda i: (last(i), 0)
    chunk_lanes = lambda i: (0, last(i))
    wide = lambda n: full((n, channels))
    input_grad, tail, returned, sums, step_grad = call(
        functools.partial(outer_kernel, group),
        [
            skip_gain, *ending, features, side_features, steps, cums, scan_grad, scaled_grad,
            score_grad, carried, entered, gated_sums, direct_sums, step_rows, head_sides, norm_grad, slope, raw, halo, filter_taps, side_slope, raw, halo, filter_taps,
        ],
        [SMEM] + [full(entry_shape)] * group
        + [
            pl.BlockSpec((rows, tokens), chunk_rows), full((side, tokens)),
            full(heads_shape), full(heads_shape),
            pl.BlockSpec((rows, tokens), chunk_rows),
            pl.BlockSpec((rows, tokens), chunk_rows),
            full((tokens, tokens)), full((state, tokens)),
            pl.BlockSpec((rows, state), chunk_rows),
            full(heads_shape), full(heads_shape), full(heads_shape), full(sides_shape),
        ]
        + [pl.BlockSpec((n, rows), chunk_lanes) for n in (8, tokens, tokens, 8, taps_count)]
        + [full((tokens, side))]
        + [pl.BlockSpec((n, side), at_side) for n in (tokens, 8, taps_count)],
        [shaped((tokens, channels), BF16)] + [shaped((8, channels))] * 3 + [shaped(heads_shape)],
        [wide(tokens), wide(8), wide(8), wide(8), full(heads_shape)],
        grid=(group + 1,), after=(coded,),
        scratch=[pltpu.VMEM((state, tokens), F32)] + [pltpu.VMEM(heads_shape, F32)] * 2
        + [pltpu.VMEM((heads, state), F32)],
    )
    returned = lax.ppermute(returned, "seq", [(s, s - 1) for s in range(1, seq)])

    there = [swap(coded, 1, 0), swap(jnp.stack(gathered[1:]), 1, 0)]

    def decode(parts, other, joined, before, after):
        specs = [full(part.shape) for part in parts]
        return call(
            functools.partial(decode_kernel, peers, other, joined), [*parts, *before],
            specs + [any_space] * len(before),
            shaped((rows, width)), any_space, after=after,
            scratch=[pltpu.VMEM((rows // 2, width), F32), pltpu.SemaphoreType.DMA((peers,))],
            aliases={len(parts): 0} if before else None,
        )

    weight_grad = decode(gathered, 0, False, (), (there[0],))
    weight_grad = decode(there, 1, True, (weight_grad,), ())

    def add_up(value, move, bits):
        while bits:
            if len(bits) > 1:
                one, two, rest = bits[0], bits[1], bits[2:]
                near, far_one = move(value, one), move(value, two)
                value = (value + near) + (far_one + move(value, one | two))
            else:
                rest = bits[1:]
                value = value + move(value, bits[0])
            bits = rest
        return value

    powers = lambda count, first: [1 << n for n in range(first, count.bit_length() - 1)]
    sums = add_up(sums, lambda v, k: swap(v, 0, k), powers(dp, 0))
    sums = add_up(sums, lambda v, k: swap(v, k, 0), powers(seq, 1))
    sums = sums + swap(sums, 1, 0)
    input_grad = lax.dynamic_update_slice_in_dim(
        input_grad, (tail + returned).astype(BF16), tokens - 8, axis=0
    )
    above = taps_count + 1
    head_at = inner + state
    return (
        input_grad[None],
        gate_grad[None],
        step_grad[None],
        weight_grad,
        sums[:above],
        sums[above, :inner],
        sums[above : above + 3, head_at : head_at + heads],
    )


def low_order(dp):
    far = dp // 2
    alone = [dp, far, dp + 1, far + 1]
    rest = [n for n in range(2, 2 * dp) if n not in alone]
    return alone + rest + [1]


def solution(mesh):
    return jax.shard_map(
        body,
        mesh=mesh,
        in_specs=(
            P("dp", "seq", None),
            P("dp", "seq", None),
            P("dp", None, "seq"),
            P(),
            P(),
            P(),
            P(),
            P(),
            P(),
            P("dp", None),
            P("dp", "seq", None),
        ),
        out_specs=(
            P("dp", "seq", None),
            P("dp", "seq", None),
            P("dp", None, "seq"),
            P("dp", None),
            P(),
            P(),
            P(),
        ),
        check_vma=False,
    )
```
